32 devices in a mesh: data: 1 (over z), tp: 4 (over y), ep: 8 (over x, core).
Axes of the slice: x: 4, y: 4, z: 1, core: 2. Of those that a mesh axis runs over, the one named last changes fastest.
The devices are a block of a 4x4x8 slice.
Arguments:
- tokens_a: bfloat16 [8192, 1536], P(('data', 'ep', 'tp'))
- tokens_b: bfloat16 [8192, 1536], P(('data', 'ep', 'tp'))
- experts_a: int32 [8192, 6], P(('data', 'ep', 'tp'))
- experts_b: int32 [8192, 6], P(('data', 'ep', 'tp'))
- gates_a: float32 [8192, 6], P(('data', 'ep', 'tp'))
- gates_b: float32 [8192, 6], P(('data', 'ep', 'tp'))
- slots_a: int32 [8192, 6], P(('data', 'ep', 'tp'))
- slots_b: int32 [8192, 6], P(('data', 'ep', 'tp'))
- shared_w1: bfloat16 [1536, 1024], P(None, 'tp')
- shared_w3: bfloat16 [1536, 1024], P(None, 'tp')
- shared_w2: bfloat16 [1024, 1536], P('tp')
- routed_w1: bfloat16 [64, 1536, 512], P('ep')
- routed_w3: bfloat16 [64, 1536, 512], P('ep')
- routed_w2: bfloat16 [64, 512, 1536], P('ep')
Outputs:
- output 1: bfloat16 [8192, 1536], P(('data', 'ep', 'tp'))
- output 2: bfloat16 [8192, 1536], P(('data', 'ep', 'tp'))
All inputs are finite; a program needn't handle non-finite values.
Results may differ from the reference program's by a relative error of at most 0.00607059.
Values are sent between devices in bfloat16 or wider.
A program may use at most 768 MiB of HBM per device.

```python
import jax
import jax.numpy as jnp
from jax import lax

TOK_DEV = 256
TP_SIZE = 4
EP_SIZE = 8
MODEL_DIM = 1536
EXPERTS = 64
TOP_K = 6
EXPERT_FF = 512
SHARED_FF = 1024
CAPACITY = 48

GROUP_DEVS = TP_SIZE * EP_SIZE
GROUP_TOK = GROUP_DEVS * TOK_DEV


def draw_routing(key):
    key_base, key_rank, key_tie = jax.random.split(key, 3)
    base = jax.random.randint(key_base, (GROUP_TOK, EXPERTS), 0, 64)
    rank_of = jax.random.permutation(key_rank, EXPERTS)
    favoured = jnp.where((rank_of >= 1) & (rank_of <= EXPERTS // 8), 6, 0)
    forced = jnp.where(rank_of == 0, 4096, 0)
    tok_ids = jnp.arange(GROUP_TOK)
    head_tok = (tok_ids % TOK_DEV) < CAPACITY
    cover = jnp.where(tok_ids[:, None] == jnp.arange(EXPERTS)[None, :], 4096, 0)
    score = base + favoured[None, :] + jnp.where(head_tok[:, None], forced[None, :], 0) + cover
    tie_rank = jax.random.permutation(key_tie, jnp.broadcast_to(jnp.arange(EXPERTS), (GROUP_TOK, EXPERTS)), axis=1, independent=True)
    chosen = lax.top_k(score * EXPERTS + tie_rank, TOP_K)[1]
    per_dev = chosen.reshape(GROUP_DEVS, TOK_DEV * TOP_K)
    one_hot = (per_dev[:, :, None] == jnp.arange(EXPERTS)[None, None, :]).astype(jnp.int32)
    earlier = jnp.cumsum(one_hot, axis=1) - one_hot
    position = jnp.sum(earlier * one_hot, axis=2)
    slots = jnp.where(position < CAPACITY, position, -1).reshape(GROUP_TOK, TOP_K)
    return chosen.astype(jnp.int32), slots.astype(jnp.int32)


def setup_inputs(seed: int = 0, part: int = 0) -> dict:
    key = jax.random.key(seed)
    part_keys = jax.random.split(jax.random.fold_in(key, part), 6)
    weight_keys = jax.random.split(key, 6)
    tokens_a = jax.random.normal(part_keys[0], (GROUP_TOK, MODEL_DIM), jnp.float32).astype(jnp.bfloat16)
    tokens_b = jax.random.normal(part_keys[1], (GROUP_TOK, MODEL_DIM), jnp.float32).astype(jnp.bfloat16)
    experts_a, slots_a = draw_routing(part_keys[2])
    experts_b, slots_b = draw_routing(part_keys[3])
    gates_a = jax.random.uniform(part_keys[4], (GROUP_TOK, TOP_K), jnp.float32, 0.5, 1.5) * TOP_K ** -0.5
    gates_b = jax.random.uniform(part_keys[5], (GROUP_TOK, TOP_K), jnp.float32, 0.5, 1.5) * TOP_K ** -0.5
    shared_w1 = (jax.random.normal(weight_keys[0], (MODEL_DIM, SHARED_FF), jnp.float32) * MODEL_DIM ** -0.5).astype(jnp.bfloat16)
    shared_w3 = (jax.random.normal(weight_keys[1], (MODEL_DIM, SHARED_FF), jnp.float32) * MODEL_DIM ** -0.5).astype(jnp.bfloat16)
    shared_w2 = (jax.random.normal(weight_keys[2], (SHARED_FF, MODEL_DIM), jnp.float32) * SHARED_FF ** -0.5).astype(jnp.bfloat16)
    routed_w1 = (jax.random.normal(weight_keys[3], (EXPERTS, MODEL_DIM, EXPERT_FF), jnp.float32) * MODEL_DIM ** -0.5).astype(jnp.bfloat16)
    routed_w3 = (jax.random.normal(weight_keys[4], (EXPERTS, MODEL_DIM, EXPERT_FF), jnp.float32) * MODEL_DIM ** -0.5).astype(jnp.bfloat16)
    routed_w2 = (jax.random.normal(weight_keys[5], (EXPERTS, EXPERT_FF, MODEL_DIM), jnp.float32) * EXPERT_FF ** -0.5).astype(jnp.bfloat16)
    return {'tokens_a': tokens_a, 'tokens_b': tokens_b, 'experts_a': experts_a, 'experts_b': experts_b, 'gates_a': gates_a, 'gates_b': gates_b, 'slots_a': slots_a, 'slots_b': slots_b, 'shared_w1': shared_w1, 'shared_w3': shared_w3, 'shared_w2': shared_w2, 'routed_w1': routed_w1, 'routed_w3': routed_w3, 'routed_w2': routed_w2}


def swiglu_rows(rows, w_in, w_gate, w_out):
    proj_in = jnp.dot(rows, w_in, preferred_element_type=jnp.float32)
    proj_gate = jnp.dot(rows, w_gate, preferred_element_type=jnp.float32)
    hidden = (jax.nn.silu(proj_in) * proj_gate).astype(jnp.bfloat16)
    return jnp.dot(hidden, w_out, preferred_element_type=jnp.float32)


def shared_expert(tokens, shared_w1, shared_w3, shared_w2):
    blocks = tokens.reshape(GROUP_DEVS, TOK_DEV, MODEL_DIM)
    result = lax.map(lambda token_block: swiglu_rows(token_block, shared_w1, shared_w3, shared_w2), blocks)
    return result.reshape(GROUP_TOK, MODEL_DIM)


def routed_experts(tokens, experts, gates, slots, routed_w1, routed_w3, routed_w2):
    tok_dev = tokens.reshape(GROUP_DEVS, TOK_DEV, MODEL_DIM).astype(jnp.float32)
    expert_dev = experts.reshape(GROUP_DEVS, TOK_DEV, TOP_K)
    slot_dev = slots.reshape(GROUP_DEVS, TOK_DEV, TOP_K)
    gate_dev = gates.reshape(GROUP_DEVS, TOK_DEV, TOP_K)
    slot_range = jnp.arange(CAPACITY)

    def one_expert(routed_acc, step_in):
        w_in, w_gate, w_out, expert = step_in
        hits = ((expert_dev == expert)[..., None] & (slot_dev[..., None] == slot_range)).astype(jnp.float32)
        place_mat = jnp.sum(hits, axis=2)
        gate_mat = jnp.sum(hits * gate_dev[..., None], axis=2)
        buffer_rows = jnp.einsum('ntc,ntd->ncd', place_mat, tok_dev).astype(jnp.bfloat16)
        expert_out = swiglu_rows(buffer_rows.reshape(GROUP_DEVS * CAPACITY, MODEL_DIM), w_in, w_gate, w_out).astype(jnp.bfloat16)
        expert_out = expert_out.reshape(GROUP_DEVS, CAPACITY, MODEL_DIM).astype(jnp.float32)
        return routed_acc + jnp.einsum('ntc,ncd->ntd', gate_mat, expert_out), None

    start_acc = jnp.zeros((GROUP_DEVS, TOK_DEV, MODEL_DIM), jnp.float32)
    routed_acc, unused = lax.scan(one_expert, start_acc, (routed_w1, routed_w3, routed_w2, jnp.arange(EXPERTS)))
    return routed_acc.reshape(GROUP_TOK, MODEL_DIM)


def one_microbatch(tokens, experts, gates, slots, shared_w1, shared_w3, shared_w2, routed_w1, routed_w3, routed_w2):
    shared_out = shared_expert(tokens, shared_w1, shared_w3, shared_w2)
    routed_out = routed_experts(tokens, experts, gates, slots, routed_w1, routed_w3, routed_w2)
    return (tokens.astype(jnp.float32) + shared_out + routed_out).astype(jnp.bfloat16)


def reference(tokens_a, tokens_b, experts_a, experts_b, gates_a, gates_b, slots_a, slots_b, shared_w1, shared_w3, shared_w2, routed_w1, routed_w3, routed_w2):
    out_a = one_microbatch(tokens_a, experts_a, gates_a, slots_a, shared_w1, shared_w3, shared_w2, routed_w1, routed_w3, routed_w2)
    out_b = one_microbatch(tokens_b, experts_b, gates_b, slots_b, shared_w1, shared_w3, shared_w2, routed_w1, routed_w3, routed_w2)
    return (out_a, out_b)
```

```python
import functools

import jax
import jax.numpy as jnp
from jax import lax
from jax.experimental import pallas as pl
from jax.experimental.pallas import tpu as pltpu
from jax.sharding import PartitionSpec as P

MESH = pl.DeviceIdType.MESH
CORES = 2
TOP_ROWS = 8
FAR, NEXT, PREV, OWN = 0, 1, 2, 3
SERVICE_AT = 4


def capacity_rows(tok_local, top_k, num_experts):
    return max(4, (2 * tok_local * top_k) // num_experts)


def split_three(value):
    hi = value.astype(jnp.bfloat16)
    rest = value - hi.astype(jnp.float32)
    mid = rest.astype(jnp.bfloat16)
    low = (rest - mid.astype(jnp.float32)).astype(jnp.bfloat16)
    return hi, mid, low


def layer_kernel(cfg, meta_in, ta, tb, s1, s3, s2, w1, w3, w2, out_a, out_b, g1, g3, g2,
                 tok, meta, xr, rp, w1b, w3b, w2b, part, rs1, rfull,
                 loc_sem, w_sem, tx_send, tx_recv, tp_send, tp_recv, mt_send, mt_recv,
                 y_send, y_recv, r_send, r_recv, c_send, c_recv, out_sem, free_sem):
    top_k, ep_size, tp_size, cap = cfg
    n_loc = w1.shape[0]
    ff = w1.shape[2]
    sh = s1.shape[1]
    rows, width = ta.shape
    half = rows // 2
    exp_rows = n_loc * cap
    nx = ep_size // CORES
    ep = lax.axis_index('ep')
    ty = lax.axis_index('tp')
    core = ep % CORES
    chip = ep // CORES
    partner = chip * CORES + (1 - core)
    x_next = ((chip + 1) % nx) * CORES + core
    x_prev = ((chip + nx - 1) % nx) * CORES + core
    y_next = (ty + 1) % tp_size
    y_prev = (ty + tp_size - 1) % tp_size
    to_xn, to_xp, to_pr = {'ep': x_next}, {'ep': x_prev}, {'ep': partner}
    to_yn, to_yp = {'tp': y_next}, {'tp': y_prev}
    lo, hi = pl.ds(0, half), pl.ds(half, half)

    def remote(src, dst, ssem, rsem, dev):
        return pltpu.make_async_remote_copy(src_ref=src, dst_ref=dst, send_sem=ssem, recv_sem=rsem,
                                            device_id=dev, device_id_type=MESH)

    def own_sends(m):
        return [remote(tok.at[m, OWN, lo], tok.at[m, PREV, lo], tx_send.at[m, 0], tx_recv.at[m, 0], to_xn),
                remote(tok.at[m, OWN, hi], tok.at[m, NEXT, hi], tx_send.at[m, 3], tx_recv.at[m, 3], to_xp),
                remote(tok.at[m, OWN, hi], tok.at[m, PREV, hi], tx_send.at[m, 1], tx_recv.at[m, 1], to_xn),
                remote(tok.at[m, OWN, lo], tok.at[m, NEXT, lo], tx_send.at[m, 2], tx_recv.at[m, 2], to_xp)]

    def forwards(m):
        return [remote(tok.at[m, PREV, lo], tok.at[m, FAR, lo], tx_send.at[m, 4], tx_recv.at[m, 4], to_xn),
                remote(tok.at[m, NEXT, hi], tok.at[m, FAR, hi], tx_send.at[m, 5], tx_recv.at[m, 5], to_xp)]

    def to_partner(m, k):
        return remote(tok.at[m, k], tok.at[m, k + 4], tp_send.at[m, k], tp_recv.at[m, k], to_pr)

    meta_next = remote(meta.at[OWN], meta.at[PREV], mt_send.at[0], mt_recv.at[0], to_xn)
    meta_prev = remote(meta.at[OWN], meta.at[NEXT], mt_send.at[1], mt_recv.at[1], to_xp)
    meta_far = remote(meta.at[PREV], meta.at[FAR], mt_send.at[2], mt_recv.at[2], to_xn)
    meta_pair = [remote(meta.at[k], meta.at[k + 4], mt_send.at[3 + k], mt_recv.at[3 + k], to_pr) for k in range(4)]
    y_own = []
    for i, (src, dst) in enumerate(((s1, g1), (s2, g2), (s3, g3))):
        y_own.append(remote(src, dst.at[PREV], y_send.at[i], y_recv.at[i], to_yn))
        y_own.append(remote(src, dst.at[NEXT], y_send.at[3 + i], y_recv.at[3 + i], to_yp))
    y_far = [remote(g1.at[PREV], g1.at[FAR], y_send.at[6], y_recv.at[6], to_yn),
             remote(g2.at[PREV], g2.at[FAR], y_send.at[7], y_recv.at[7], to_yn),
             remote(g3.at[NEXT], g3.at[FAR], y_send.at[8], y_recv.at[8], to_yp)]

    def weights(e, slot):
        return [pltpu.make_async_copy(w1.at[e], w1b.at[slot], w_sem.at[slot, 0]),
                pltpu.make_async_copy(w3.at[e], w3b.at[slot], w_sem.at[slot, 1]),
                pltpu.make_async_copy(w2.at[e], w2b.at[slot], w_sem.at[slot, 2])]

    def push_rows(m, e):
        return remote(xr.at[e, pl.ds(4, 4)], rp.at[e], r_send.at[m, e], r_recv.at[m, e], to_pr)

    def first_far(m):
        return [remote(part.at[m, FAR, hi], rs1.at[m, 0], c_send.at[m, 0], c_recv.at[m, 0], to_xn),
                remote(part.at[m, FAR, lo], rs1.at[m, 1], c_send.at[m, 1], c_recv.at[m, 1], to_xp)]

    def near_own(m):
        return [remote(part.at[m, NEXT, lo], rfull.at[m, 0, lo], c_send.at[m, 2], c_recv.at[m, 2], to_xn),
                remote(part.at[m, PREV, hi], rfull.at[m, 1, hi], c_send.at[m, 3], c_recv.at[m, 3], to_xp)]

    def near_sum(m):
        return [remote(part.at[m, NEXT, hi], rfull.at[m, 0, hi], c_send.at[m, 4], c_recv.at[m, 4], to_xn),
                remote(part.at[m, PREV, lo], rfull.at[m, 1, lo], c_send.at[m, 5], c_recv.at[m, 5], to_xp)]

    local = [pltpu.make_async_copy(meta_in, meta.at[OWN], loc_sem.at[0]),
             pltpu.make_async_copy(ta, tok.at[0, OWN], loc_sem.at[1]),
             pltpu.make_async_copy(tb, tok.at[1, OWN], loc_sem.at[2])]
    for cp in local + weights(0, 0):
        cp.start()
    barrier = pltpu.get_barrier_semaphore()
    for dev in (to_xn, to_xp, to_pr, to_yn, to_yp):
        pl.semaphore_signal(barrier, inc=1, device_id=dev, device_id_type=MESH)
    for cp in local:
        cp.wait()
    pl.semaphore_wait(barrier, 5)

    for cp in [meta_next, meta_prev, meta_pair[OWN]] + own_sends(0) + [to_partner(0, OWN)]:
        cp.start()
    for cp in y_own:
        cp.start()
    sent = own_sends(0)
    sent[0].wait_recv()
    sent[1].wait_recv()
    for cp in forwards(0):
        cp.start()
    meta_next.wait_recv()
    meta_prev.wait_recv()
    meta_far.start()
    for cp in own_sends(1) + [to_partner(1, OWN), meta_pair[NEXT], meta_pair[PREV]]:
        cp.start()
    sent[2].wait_recv()
    sent[3].wait_recv()
    to_partner(0, NEXT).start()
    to_partner(0, PREV).start()
    meta_far.wait_recv()
    meta_pair[FAR].start()
    for cp in forwards(0):
        cp.wait_recv()
    to_partner(0, FAR).start()
    for k in range(4):
        meta_pair[k].wait_recv()
        to_partner(0, k).wait_recv()

    row_id = lax.broadcasted_iota(jnp.int32, (exp_rows, rows), 0).astype(jnp.float32)

    def placed(ids, base, values):
        shifted = row_id + (base * exp_rows).astype(jnp.float32)
        total = jnp.zeros((exp_rows, rows), jnp.float32)
        for j in range(top_k):
            total = jnp.where(shifted == ids[j:j + 1, :], 1.0 if values is None else values[j:j + 1, :], total)
        return total

    def gather(m):
        def one(k, carry):
            ids = meta[k, m, pl.ds(0, TOP_ROWS), :]
            place = placed(ids, ep, None).astype(jnp.bfloat16)
            got = jnp.dot(place, tok[m, k], preferred_element_type=jnp.float32).astype(jnp.bfloat16)
            xr[:, k] = got.reshape(n_loc, cap, width)
            return carry
        lax.fori_loop(0, 8, one, 0)

    def swiglu(x_rows, slot):
        proj_in = jnp.dot(x_rows, w1b[slot], preferred_element_type=jnp.float32)
        proj_gate = jnp.dot(x_rows, w3b[slot], preferred_element_type=jnp.float32)
        hidden = (jax.nn.silu(proj_in) * proj_gate).astype(jnp.bfloat16)
        return jnp.dot(hidden, w2b[slot], preferred_element_type=jnp.float32)

    def experts(m):
        def one(e, carry):
            slot = e % 2

            def prefetch():
                for cp in weights((e + 1) % n_loc, 1 - slot):
                    cp.start()
            if m == 0:
                prefetch()
            else:
                pl.when(e < n_loc - 1)(prefetch)

            @pl.when(e > 0)
            def _():
                push_rows(m, e - 1).start()
            for cp in weights(e, slot):
                cp.wait()
            res = swiglu(xr[e].reshape(8 * cap, width), slot).astype(jnp.bfloat16)
            xr[e] = res.reshape(8, cap, width)
            if m == 0:
                @pl.when(e == SERVICE_AT)
                def _():
                    s = own_sends(1)
                    s[0].wait_recv()
                    s[1].wait_recv()
                    for cp in forwards(1):
                        cp.start()
                    s[2].wait_recv()
                    s[3].wait_recv()
                    to_partner(1, NEXT).start()
                    to_partner(1, PREV).start()
            return carry
        lax.fori_loop(0, n_loc, one, 0)
        push_rows(m, n_loc - 1).start()

    def combine(m):
        for e in range(n_loc):
            push_rows(m, e).wait_recv()

        def one(i, carry):
            ids = meta[i, m, pl.ds(0, TOP_ROWS), :]
            vals = meta[i, m, pl.ds(TOP_ROWS, TOP_ROWS), :]
            mine = jnp.concatenate(split_three(placed(ids, ep, vals).T), axis=0)
            other = jnp.concatenate(split_three(placed(ids, partner, vals).T), axis=0)
            for n in range(width // 256):
                cols = pl.ds(n * 256, 256)
                acc = jnp.dot(mine, xr[:, i, :, cols].reshape(exp_rows, 256), preferred_element_type=jnp.float32)
                acc = acc + jnp.dot(other, rp[:, i, :, cols].reshape(exp_rows, 256), preferred_element_type=jnp.float32)
                part[m, i, :, cols] = acc[0:rows] + acc[rows:2 * rows] + acc[2 * rows:3 * rows]

            @pl.when(i == 1)
            def _():
                for cp in first_far(m):
                    cp.start()

            @pl.when(i == 2)
            def _():
                near_own(m)[0].start()

            @pl.when(i == 3)
            def _():
                near_own(m)[1].start()
            return carry
        lax.fori_loop(0, 4, one, 0)

    def pass_on(m):
        first = first_far(m)
        sends = near_sum(m)
        first[0].wait_recv()
        part[m, NEXT, hi] = part[m, NEXT, hi] + rs1[m, 0]
        first[1].wait_recv()
        part[m, PREV, lo] = part[m, PREV, lo] + rs1[m, 1]
        sends[0].start()
        sends[1].start()

    def finish(m, out):
        for cp in own_sends(m) + [to_partner(m, OWN)]:
            cp.wait_send()
        for cp in near_own(m) + near_sum(m):
            cp.wait_recv()
        total = part[m, OWN] + tok[m, OWN].astype(jnp.float32) + rfull[m, 0] + rfull[m, 1]
        tok[m, OWN] = total.astype(jnp.bfloat16)
        cp = pltpu.make_async_copy(tok.at[m, OWN], out, out_sem.at[m])
        cp.start()
        return cp

    gather(0)
    experts(0)
    for cp in forwards(1):
        cp.wait_recv()
    to_partner(1, FAR).start()
    combine(0)
    pl.semaphore_signal(free_sem, inc=1, device_id=to_pr, device_id_type=MESH)
    for cp in y_own:
        cp.wait_recv()
    for cp in y_far:
        cp.start()
    for k in range(4):
        to_partner(1, k).wait_recv()
    for e in range(n_loc):
        push_rows(0, e).wait_send()
    gather(1)
    pl.semaphore_wait(free_sem, 1)
    experts(1)
    pass_on(0)
    for cp in y_far:
        cp.wait_recv()
    shared = []
    for slot, pair in enumerate((((s1, s3, s2), NEXT), (None, FAR))):
        srcs = [pair[0] or (g1.at[PREV], g3.at[PREV], g2.at[PREV]), (g1.at[pair[1]], g3.at[pair[1]], g2.at[pair[1]])]
        for p, (a1, a3, a2) in enumerate(srcs):
            part_of = pl.ds(p * sh, sh)
            shared.append(pltpu.make_async_copy(a1, w1b.at[slot, :, part_of], w_sem.at[slot, 3 + p]))
            shared.append(pltpu.make_async_copy(a3, w3b.at[slot, :, part_of], w_sem.at[slot, 5 + p]))
            shared.append(pltpu.make_async_copy(a2, w2b.at[slot, part_of, :], w_sem.at[slot, 7 + p]))
    for cp in shared:
        cp.start()
    combine(1)
    for cp in shared:
        cp.wait()

    def shared_one(i, carry):
        m = i // 2
        part[m, OWN] = part[m, OWN] + swiglu(tok[m, OWN], i % 2)
        return carry
    lax.fori_loop(0, 4, shared_one, 0)

    done_a = finish(0, out_a)
    pass_on(1)
    done_b = finish(1, out_b)
    for m in range(2):
        for k in range(3):
            to_partner(m, k).wait_send()
        for cp in forwards(m) + first_far(m) + near_own(m) + near_sum(m):
            cp.wait_send()
    for e in range(n_loc):
        push_rows(1, e).wait_send()
    for cp in [meta_next, meta_prev, meta_far] + meta_pair + y_own + y_far:
        cp.wait_send()
    done_a.wait()
    done_b.wait()


def solution(mesh):
    ep_size = mesh.shape['ep']
    tp_size = mesh.shape['tp']
    tok_spec = P(('data', 'ep', 'tp'), None)
    in_specs = (tok_spec,) * 8 + (P(None, 'tp'), P(None, 'tp'), P('tp', None), P('ep', None, None), P('ep', None, None), P('ep', None, None))

    def routing_rows(expert_ids, gate_vals, slot_ids, cap):
        keep = slot_ids >= 0
        ids = jnp.where(keep, expert_ids * cap + slot_ids, -1).astype(jnp.float32).T
        vals = jnp.where(keep, gate_vals, 0.0).T
        pad = ((0, TOP_ROWS - ids.shape[0]), (0, 0))
        return jnp.concatenate([jnp.pad(ids, pad, constant_values=-1.0), jnp.pad(vals, pad)], axis=0)

    def layer_local(tokens_a, tokens_b, experts_a, experts_b, gates_a, gates_b, slots_a, slots_b, shared_w1, shared_w3, shared_w2, routed_w1, routed_w3, routed_w2):
        rows, width = tokens_a.shape
        top_k = experts_a.shape[1]
        n_loc, _, ff = routed_w1.shape
        sh = shared_w1.shape[1]
        cap = capacity_rows(rows, top_k, n_loc * ep_size)
        half = rows // 2
        meta = jnp.stack([routing_rows(experts_a, gates_a, slots_a, cap), routing_rows(experts_b, gates_b, slots_b, cap)])
        bf, f32 = jnp.bfloat16, jnp.float32
        dma = pltpu.SemaphoreType.DMA
        any_spec = pl.BlockSpec(memory_space=pl.ANY)
        outs = pl.pallas_call(
            functools.partial(layer_kernel, (top_k, ep_size, tp_size, cap)),
            out_shape=(jax.ShapeDtypeStruct((rows, width), bf), jax.ShapeDtypeStruct((rows, width), bf),
                       jax.ShapeDtypeStruct((3, width, sh), bf), jax.ShapeDtypeStruct((3, width, sh), bf),
                       jax.ShapeDtypeStruct((3, sh, width), bf)),
            in_specs=[any_spec] * 9,
            out_specs=[any_spec] * 5,
            scratch_shapes=[
                pltpu.VMEM((2, 8, rows, width), bf),
                pltpu.VMEM((8, 2, 2 * TOP_ROWS, rows), f32),
                pltpu.VMEM((n_loc, 8, cap, width), bf),
                pltpu.VMEM((n_loc, 4, cap, width), bf),
                pltpu.VMEM((2, width, ff), bf),
                pltpu.VMEM((2, width, ff), bf),
                pltpu.VMEM((2, ff, width), bf),
                pltpu.VMEM((2, 4, rows, width), f32),
                pltpu.VMEM((2, 2, half, width), f32),
                pltpu.VMEM((2, 2, rows, width), f32),
                dma((3,)), dma((2, 9)), dma((2, 6)), dma((2, 6)), dma((2, 4)), dma((2, 4)), dma((7,)), dma((7,)),
                dma((9,)), dma((9,)), dma((2, n_loc)), dma((2, n_loc)), dma((2, 6)), dma((2, 6)), dma((2,)),
                pltpu.SemaphoreType.REGULAR,
            ],
            compiler_params=pltpu.CompilerParams(collective_id=0, has_side_effects=True, vmem_limit_bytes=67043328),
        )(meta, tokens_a, tokens_b, shared_w1, shared_w3, shared_w2, routed_w1, routed_w3, routed_w2)
        return outs[0], outs[1]

    return jax.shard_map(layer_local, mesh=mesh, in_specs=in_specs, out_specs=(tok_spec, tok_spec), check_vma=False)
```

```python
import functools

import jax
import jax.numpy as jnp
from jax import lax
from jax.experimental import pallas as pl
from jax.experimental.pallas import tpu as pltpu
from jax.sharding import PartitionSpec as P

MESH = pl.DeviceIdType.MESH
CORES = 2
OWN, NEXT, PREV, FAR = 0, 1, 2, 3


def capacity_rows(tok_local, top_k, num_experts):
    return max(4, (2 * tok_local * top_k) // num_experts)


def split_three(value):
    hi = value.astype(jnp.bfloat16)
    rest = value - hi.astype(jnp.float32)
    mid = rest.astype(jnp.bfloat16)
    low = (rest - mid.astype(jnp.float32)).astype(jnp.bfloat16)
    return hi, mid, low


def layer_kernel(cfg, ea, eb, ga, gb, sa, sb, ta, tb, s1, s3, s2, w1, w3, w2, out_a, out_b, g1, g3, g2,
                 tok, mids, mval, xr, rp, w1b, w3b, w2b, part, rs1, rfull,
                 loc_sem, w_sem, tx_send, tx_recv, tp_send, tp_recv, mt_send, mt_recv,
                 y_send, y_recv, r_send, r_recv, c_send, c_recv, out_sem, free_sem):
    top_k, ep_size, tp_size, cap = cfg
    n_loc = w1.shape[0]
    ff = w1.shape[2]
    sh = s1.shape[1]
    rows, width = ta.shape
    half = rows // 2
    exp_rows = n_loc * cap
    nx = ep_size // CORES
    ep = lax.axis_index('ep')
    ty = lax.axis_index('tp')
    core = ep % CORES
    chip = ep // CORES
    partner = chip * CORES + (1 - core)
    x_next = ((chip + 1) % nx) * CORES + core
    x_prev = ((chip + nx - 1) % nx) * CORES + core
    y_next = (ty + 1) % tp_size
    y_prev = (ty + tp_size - 1) % tp_size
    to_xn, to_xp, to_pr = {'ep': x_next}, {'ep': x_prev}, {'ep': partner}
    to_yn, to_yp = {'tp': y_next}, {'tp': y_prev}
    lo, hi = pl.ds(0, half), pl.ds(half, half)

    def remote(src, dst, ssem, rsem, dev):
        return pltpu.make_async_remote_copy(src_ref=src, dst_ref=dst, send_sem=ssem, recv_sem=rsem,
                                            device_id=dev, device_id_type=MESH)

    def own_sends(m):
        return [remote(tok.at[m, OWN, lo], tok.at[m, PREV, lo], tx_send.at[m, 0], tx_recv.at[m, 0], to_xn),
                remote(tok.at[m, OWN, hi], tok.at[m, NEXT, hi], tx_send.at[m, 3], tx_recv.at[m, 3], to_xp),
                remote(tok.at[m, OWN, hi], tok.at[m, PREV, hi], tx_send.at[m, 1], tx_recv.at[m, 1], to_xn),
                remote(tok.at[m, OWN, lo], tok.at[m, NEXT, lo], tx_send.at[m, 2], tx_recv.at[m, 2], to_xp)]

    def forwards(m):
        return [remote(tok.at[m, PREV, lo], tok.at[m, FAR, lo], tx_send.at[m, 4], tx_recv.at[m, 4], to_xn),
                remote(tok.at[m, NEXT, hi], tok.at[m, FAR, hi], tx_send.at[m, 5], tx_recv.at[m, 5], to_xp)]

    def to_partner(m, k):
        return remote(tok.at[m, k], tok.at[m, k + 4], tp_send.at[m, k], tp_recv.at[m, k], to_pr)

    def meta(i, src, dst, dev):
        return [remote(mids.at[src], mids.at[dst], mt_send.at[0, i], mt_recv.at[0, i], dev),
                remote(mval.at[src], mval.at[dst], mt_send.at[1, i], mt_recv.at[1, i], dev)]

    meta_next = meta(0, OWN, PREV, to_xn)
    meta_prev = meta(1, OWN, NEXT, to_xp)
    meta_far = meta(2, PREV, FAR, to_xn)
    meta_pair = [meta(3 + k, k, k + 4, to_pr) for k in range(4)]
    y_own = []
    for i, (src, dst) in enumerate(((s1, g1), (s2, g2), (s3, g3))):
        y_own.append(remote(src, dst.at[PREV - 1], y_send.at[i], y_recv.at[i], to_yn))
        y_own.append(remote(src, dst.at[NEXT - 1], y_send.at[3 + i], y_recv.at[3 + i], to_yp))
    y_far = [remote(g1.at[PREV - 1], g1.at[FAR - 1], y_send.at[6], y_recv.at[6], to_yn),
             remote(g2.at[PREV - 1], g2.at[FAR - 1], y_send.at[7], y_recv.at[7], to_yn),
             remote(g3.at[NEXT - 1], g3.at[FAR - 1], y_send.at[8], y_recv.at[8], to_yp)]

    def weights(e, slot):
        return [pltpu.make_async_copy(w1.at[e], w1b.at[slot], w_sem.at[slot, 0]),
                pltpu.make_async_copy(w3.at[e], w3b.at[slot], w_sem.at[slot, 1]),
                pltpu.make_async_copy(w2.at[e], w2b.at[slot], w_sem.at[slot, 2])]

    def push_rows(m, e):
        return remote(xr.at[e, pl.ds(4, 4)], rp.at[e], r_send.at[m, e], r_recv.at[m, e], to_pr)

    def first_far(m):
        return [remote(part.at[m, FAR, hi], rs1.at[m, 0], c_send.at[m, 0], c_recv.at[m, 0], to_xn),
                remote(part.at[m, FAR, lo], rs1.at[m, 1], c_send.at[m, 1], c_recv.at[m, 1], to_xp)]

    def near_own(m):
        return [remote(part.at[m, NEXT, lo], rfull.at[m, 0, lo], c_send.at[m, 2], c_recv.at[m, 2], to_xn),
                remote(part.at[m, PREV, hi], rfull.at[m, 1, hi], c_send.at[m, 3], c_recv.at[m, 3], to_xp)]

    def near_sum(m):
        return [remote(part.at[m, NEXT, hi], rfull.at[m, 0, hi], c_send.at[m, 4], c_recv.at[m, 4], to_xn),
                remote(part.at[m, PREV, lo], rfull.at[m, 1, lo], c_send.at[m, 5], c_recv.at[m, 5], to_xp)]

    local = [pltpu.make_async_copy(src, dst, loc_sem.at[i]) for i, (src, dst) in enumerate((
        (ta, tok.at[0, OWN]), (ea, mids.at[OWN, 0, 0]), (sa, mids.at[OWN, 0, 1]), (ga, mval.at[OWN, 0]),
        (eb, mids.at[OWN, 1, 0]), (sb, mids.at[OWN, 1, 1]), (gb, mval.at[OWN, 1]), (tb, tok.at[1, OWN])))]
    barrier = pltpu.get_barrier_semaphore()
    for dev in (to_xn, to_xp, to_pr, to_yn, to_yp):
        pl.semaphore_signal(barrier, inc=1, device_id=dev, device_id_type=MESH)
    for cp in local:
        cp.start()
    for cp in local[:-1]:
        cp.wait()
    pl.semaphore_wait(barrier, 5)
    first = own_sends(0)
    for cp in meta_next + meta_prev + first + meta_pair[OWN] + [to_partner(0, OWN)]:
        cp.start()
    for cp in y_own + weights(0, 0):
        cp.start()
    local[-1].wait()

    row_id = lax.broadcasted_iota(jnp.int32, (exp_rows, rows), 0)

    def placed(ids, base, values):
        shifted = row_id + base * exp_rows
        total = jnp.zeros((exp_rows, rows), jnp.float32)
        for j in range(top_k):
            total = jnp.where(shifted == ids[j:j + 1, :], 1.0 if values is None else values[j:j + 1, :], total)
        return total

    def row_ids(k, m):
        slot = mids[k, m, 1]
        return jnp.where(slot >= 0, mids[k, m, 0] * cap + slot, -1)

    def arrivals(step):
        if step == 1:
            for cp in meta_pair[OWN] + [to_partner(0, OWN)]:
                cp.wait_recv()
        elif step == 2:
            first[0].wait_recv()
            first[1].wait_recv()
            for cp in forwards(0):
                cp.start()
            for cp in meta_next + meta_prev:
                cp.wait_recv()
            for cp in meta_far + own_sends(1) + meta_pair[NEXT] + meta_pair[PREV] + [to_partner(1, OWN)]:
                cp.start()
            first[2].wait_recv()
            first[3].wait_recv()
            to_partner(0, NEXT).start()
            to_partner(0, PREV).start()
        elif step in (3, 5):
            k = NEXT if step == 3 else PREV
            for cp in meta_pair[k] + [to_partner(0, k)]:
                cp.wait_recv()
        elif step == 6:
            for cp in meta_far:
                cp.wait_recv()
            for cp in meta_pair[FAR]:
                cp.start()
            for cp in forwards(0):
                cp.wait_recv()
            to_partner(0, FAR).start()
        elif step == 7:
            for cp in meta_pair[FAR] + [to_partner(0, FAR)]:
                cp.wait_recv()

    def gather(m):
        def one(step, carry):
            if m == 0:
                for at in range(1, 8):
                    pl.when(step == at)(functools.partial(arrivals, at))
            k = (step % 2) * 4 + step // 2
            place = placed(row_ids(k, m), ep, None).astype(jnp.bfloat16)
            got = jnp.dot(place, tok[m, k], preferred_element_type=jnp.float32).astype(jnp.bfloat16)
            xr[:, k] = got.reshape(n_loc, cap, width)
            return carry
        lax.fori_loop(0, 8, one, 0)

    def swiglu(x_rows, slot):
        proj_in = jnp.dot(x_rows, w1b[slot], preferred_element_type=jnp.float32)
        proj_gate = jnp.dot(x_rows, w3b[slot], preferred_element_type=jnp.float32)
        hidden = (jax.nn.silu(proj_in) * proj_gate).astype(jnp.bfloat16)
        return jnp.dot(hidden, w2b[slot], preferred_element_type=jnp.float32)

    def second_arrivals(step):
        sends = own_sends(1)
        if step == 0:
            sends[0].wait_recv()
            sends[1].wait_recv()
            for cp in forwards(1):
                cp.start()
        else:
            sends[2].wait_recv()
            sends[3].wait_recv()
            to_partner(1, NEXT).start()
            to_partner(1, PREV).start()

    def experts(m):
        def one(e, carry):
            slot = e % 2

            def prefetch():
                for cp in weights((e + 1) % n_loc, 1 - slot):
                    cp.start()
            if m == 0:
                prefetch()
            else:
                pl.when(e < n_loc - 1)(prefetch)

            @pl.when(e > 0)
            def _():
                push_rows(m, e - 1).start()
            for cp in weights(e, slot):
                cp.wait()
            res = swiglu(xr[e].reshape(8 * cap, width), slot).astype(jnp.bfloat16)
            xr[e] = res.reshape(8, cap, width)
            if m == 0:
                pl.when(e == n_loc // 2 - 1)(functools.partial(second_arrivals, 0))
                pl.when(e == n_loc - 2)(functools.partial(second_arrivals, 1))
            return carry
        lax.fori_loop(0, n_loc, one, 0)
        push_rows(m, n_loc - 1).start()

    def combine(m):
        for e in range(n_loc):
            push_rows(m, e).wait_recv()

        def one(step, carry):
            i = 3 - step
            ids = row_ids(i, m)
            vals = jnp.where(mids[i, m, 1] >= 0, mval[i, m], 0.0)
            mine = jnp.concatenate(split_three(placed(ids, ep, vals).T), axis=0)
            other = jnp.concatenate(split_three(placed(ids, partner, vals).T), axis=0)
            for n in range(width // 256):
                cols = pl.ds(n * 256, 256)
                acc = jnp.dot(mine, xr[:, i, :, cols].reshape(exp_rows, 256), preferred_element_type=jnp.float32)
                acc = acc + jnp.dot(other, rp[:, i, :, cols].reshape(exp_rows, 256), preferred_element_type=jnp.float32)
                part[m, i, :, cols] = acc[0:rows] + acc[rows:2 * rows] + acc[2 * rows:3 * rows]

            @pl.when(step == 0)
            def _():
                for cp in first_far(m):
                    cp.start()

            @pl.when(step == 1)
            def _():
                near_own(m)[1].start()

            @pl.when(step == 2)
            def _():
                near_own(m)[0].start()
            return carry
        lax.fori_loop(0, 4, one, 0)

    def pass_on(m):
        incoming = first_far(m)
        sends = near_sum(m)
        incoming[0].wait_recv()
        part[m, NEXT, hi] = part[m, NEXT, hi] + rs1[m, 0]
        incoming[1].wait_recv()
        part[m, PREV, lo] = part[m, PREV, lo] + rs1[m, 1]
        sends[0].start()
        sends[1].start()

    def finish(m, out):
        for cp in own_sends(m) + [to_partner(m, OWN)]:
            cp.wait_send()
        for cp in near_own(m) + near_sum(m):
            cp.wait_recv()
        total = part[m, OWN] + tok[m, OWN].astype(jnp.float32) + rfull[m, 0] + rfull[m, 1]
        tok[m, OWN] = total.astype(jnp.bfloat16)
        cp = pltpu.make_async_copy(tok.at[m, OWN], out, out_sem.at[m])
        cp.start()
        return cp

    gather(0)
    experts(0)
    combine(0)
    for cp in forwards(1):
        cp.wait_recv()
    to_partner(1, FAR).start()
    pl.semaphore_signal(free_sem, inc=1, device_id=to_pr, device_id_type=MESH)
    for cp in y_own:
        cp.wait_recv()
    for cp in y_far:
        cp.start()
    for k in range(4):
        to_partner(1, k).wait_recv()
    for e in range(n_loc):
        push_rows(0, e).wait_send()
    gather(1)
    pl.semaphore_wait(free_sem, 1)
    experts(1)
    pass_on(0)
    for cp in y_far:
        cp.wait_recv()
    shared = []
    for slot, pair in enumerate((((s1, s3, s2), NEXT), (None, FAR))):
        srcs = [pair[0] or (g1.at[PREV - 1], g3.at[PREV - 1], g2.at[PREV - 1]), (g1.at[pair[1] - 1], g3.at[pair[1] - 1], g2.at[pair[1] - 1])]
        for p, (a1, a3, a2) in enumerate(srcs):
            part_of = pl.ds(p * sh, sh)
            shared.append(pltpu.make_async_copy(a1, w1b.at[slot, :, part_of], w_sem.at[slot, 3 + p]))
            shared.append(pltpu.make_async_copy(a3, w3b.at[slot, :, part_of], w_sem.at[slot, 5 + p]))
            shared.append(pltpu.make_async_copy(a2, w2b.at[slot, part_of, :], w_sem.at[slot, 7 + p]))
    for cp in shared:
        cp.start()
    combine(1)
    for cp in shared:
        cp.wait()

    def shared_one(i, carry):
        m = i // 2
        part[m, OWN] = part[m, OWN] + swiglu(tok[m, OWN], i % 2)
        return carry
    lax.fori_loop(0, 4, shared_one, 0)

    done_a = finish(0, out_a)
    pass_on(1)
    done_b = finish(1, out_b)
    for m in range(2):
        for k in (NEXT, PREV, FAR):
            to_partner(m, k).wait_send()
        for cp in forwards(m) + first_far(m) + near_own(m) + near_sum(m):
            cp.wait_send()
    for e in range(n_loc):
        push_rows(1, e).wait_send()
    for cp in meta_next + meta_prev + meta_far + sum(meta_pair, []) + y_own + y_far:
        cp.wait_send()
    done_a.wait()
    done_b.wait()


def place_kernel(a, b, out_a, out_b, buf, in_sem, out_sem):
    loads = [pltpu.make_async_copy(src, buf.at[i], in_sem.at[i]) for i, src in enumerate((a, b))]
    stores = [pltpu.make_async_copy(buf.at[i], dst, out_sem.at[i]) for i, dst in enumerate((out_a, out_b))]
    for cp in loads:
        cp.start()
    for load, store in zip(loads, stores):
        load.wait()
        store.start()
    for cp in stores:
        cp.wait()


def solution(mesh):
    ep_size = mesh.shape['ep']
    tp_size = mesh.shape['tp']
    tok_spec = P(('data', 'ep', 'tp'), None)
    in_specs = (tok_spec,) * 8 + (P(None, 'tp'), P(None, 'tp'), P('tp', None), P('ep', None, None), P('ep', None, None), P('ep', None, None))

    def layer_local(tokens_a, tokens_b, experts_a, experts_b, gates_a, gates_b, slots_a, slots_b, shared_w1, shared_w3, shared_w2, routed_w1, routed_w3, routed_w2):
        rows, width = tokens_a.shape
        top_k = experts_a.shape[1]
        n_loc, _, ff = routed_w1.shape
        sh = shared_w1.shape[1]
        cap = capacity_rows(rows, top_k, n_loc * ep_size)
        half = rows // 2
        routing = [a.T for a in (experts_a, experts_b, gates_a, gates_b, slots_a, slots_b)]
        bf, f32 = jnp.bfloat16, jnp.float32
        dma = pltpu.SemaphoreType.DMA
        any_spec = pl.BlockSpec(memory_space=pl.ANY)
        outs = pl.pallas_call(
            functools.partial(layer_kernel, (top_k, ep_size, tp_size, cap)),
            out_shape=(jax.ShapeDtypeStruct((rows, width), bf), jax.ShapeDtypeStruct((rows, width), bf),
                       jax.ShapeDtypeStruct((3, width, sh), bf), jax.ShapeDtypeStruct((3, width, sh), bf),
                       jax.ShapeDtypeStruct((3, sh, width), bf)),
            in_specs=[any_spec] * 14,
            out_specs=[any_spec] * 5,
            scratch_shapes=[
                pltpu.VMEM((2, 8, rows, width), bf),
                pltpu.VMEM((8, 2, 2, top_k, rows), jnp.int32),
                pltpu.VMEM((8, 2, top_k, rows), f32),
                pltpu.VMEM((n_loc, 8, cap, width), bf),
                pltpu.VMEM((n_loc, 4, cap, width), bf),
                pltpu.VMEM((2, width, ff), bf),
                pltpu.VMEM((2, width, ff), bf),
                pltpu.VMEM((2, ff, width), bf),
                pltpu.VMEM((2, 4, rows, width), f32),
                pltpu.VMEM((2, 2, half, width), f32),
                pltpu.VMEM((2, 2, rows, width), f32),
                dma((8,)), dma((2, 9)), dma((2, 6)), dma((2, 6)), dma((2, 4)), dma((2, 4)), dma((2, 7)), dma((2, 7)),
                dma((9,)), dma((9,)), dma((2, n_loc)), dma((2, n_loc)), dma((2, 6)), dma((2, 6)), dma((2,)),
                pltpu.SemaphoreType.REGULAR,
            ],
            compiler_params=pltpu.CompilerParams(collective_id=0, has_side_effects=True, vmem_limit_bytes=67043328),
        )(*routing, tokens_a, tokens_b, shared_w1, shared_w3, shared_w2, routed_w1, routed_w3, routed_w2)
        return pl.pallas_call(
            place_kernel,
            out_shape=(jax.ShapeDtypeStruct((rows, width), bf),) * 2,
            in_specs=[any_spec] * 2,
            out_specs=[any_spec] * 2,
            scratch_shapes=[pltpu.VMEM((2, rows, width), bf), dma((2,)), dma((2,))],
        )(outs[0], outs[1])

    return jax.shard_map(layer_local, mesh=mesh, in_specs=in_specs, out_specs=(tok_spec, tok_spec), check_vma=False)
```

```python
import functools

import jax
import jax.numpy as jnp
from jax import lax
from jax.experimental import pallas as pl
from jax.experimental.pallas import tpu as pltpu
from jax.sharding import PartitionSpec as P

MESH = pl.DeviceIdType.MESH
VMEM_BYTES = 65000000
CORES = 2
OWN, NEXT, PREV, FAR = 0, 1, 2, 3


def capacity_rows(tok_local, top_k, num_experts):
    return max(4, (2 * tok_local * top_k) // num_experts)


def split_three(value):
    hi = value.astype(jnp.bfloat16)
    rest = value - hi.astype(jnp.float32)
    mid = rest.astype(jnp.bfloat16)
    low = (rest - mid.astype(jnp.float32)).astype(jnp.bfloat16)
    return hi, mid, low


def layer_kernel(cfg, ea, eb, ga, gb, sa, sb, ta, tb, s1, s3, s2, w1, w3, w2, out_a, out_b, g1, g3, g2,
                 tok, routing, stage_e, stage_s, stage_g, xr, rp, w1b, w3b, w2b, part, rs1, rfull,
                 loc_sem, w_sem, tx_send, tx_recv, tp_send, tp_recv, mt_send, mt_recv,
                 y_send, y_recv, r_send, r_recv, c_send, c_recv, free_sem, y_ready):
    top_k, ep_size, tp_size, cap = cfg
    n_loc = w1.shape[0]
    ff = w1.shape[2]
    sh = s1.shape[1]
    rows, width = ta.shape
    half = rows // 2
    exp_rows = n_loc * cap
    nx = ep_size // CORES
    ep = lax.axis_index('ep')
    ty = lax.axis_index('tp')
    core = ep % CORES
    chip = ep // CORES
    partner = chip * CORES + (1 - core)
    x_next = ((chip + 1) % nx) * CORES + core
    x_prev = ((chip + nx - 1) % nx) * CORES + core
    y_next = (ty + 1) % tp_size
    y_prev = (ty + tp_size - 1) % tp_size
    to_xn, to_xp, to_pr = {'ep': x_next}, {'ep': x_prev}, {'ep': partner}
    to_yn, to_yp = {'tp': y_next}, {'tp': y_prev}
    lo, hi = pl.ds(0, half), pl.ds(half, half)

    def remote(src, dst, ssem, rsem, dev):
        return pltpu.make_async_remote_copy(src_ref=src, dst_ref=dst, send_sem=ssem, recv_sem=rsem,
                                            device_id=dev, device_id_type=MESH)

    def own_sends(m):
        mine = (ta, tb)[m]
        return [remote(mine.at[lo], tok.at[m, PREV, lo], tx_send.at[m, 0], tx_recv.at[m, 0], to_xn),
                remote(mine.at[hi], tok.at[m, NEXT, hi], tx_send.at[m, 3], tx_recv.at[m, 3], to_xp),
                remote(mine.at[hi], tok.at[m, PREV, hi], tx_send.at[m, 1], tx_recv.at[m, 1], to_xn),
                remote(mine.at[lo], tok.at[m, NEXT, lo], tx_send.at[m, 2], tx_recv.at[m, 2], to_xp)]

    def forwards(m):
        return [remote(tok.at[m, PREV, lo], tok.at[m, FAR, lo], tx_send.at[m, 4], tx_recv.at[m, 4], to_xn),
                remote(tok.at[m, NEXT, hi], tok.at[m, FAR, hi], tx_send.at[m, 5], tx_recv.at[m, 5], to_xp)]

    def to_partner(m, k):
        return remote((ta, tb)[m] if k == OWN else tok.at[m, k], tok.at[m, k + 4], tp_send.at[m, k], tp_recv.at[m, k], to_pr)

    def meta(i, src, dst, dev, lines=pl.ds(0, 4 * top_k)):
        return remote(routing.at[src, lines], routing.at[dst, lines], mt_send.at[i], mt_recv.at[i], dev)

    far_cut = (4 * top_k * 2 // 3) // 8 * 8
    meta_next = meta(0, OWN, PREV, to_xn)
    meta_prev = meta(1, OWN, NEXT, to_xp)
    meta_far = [meta(2, PREV, FAR, to_xn, pl.ds(0, far_cut)),
                meta(3, NEXT, FAR, to_xp, pl.ds(far_cut, 4 * top_k - far_cut))]
    meta_pair = [meta(4 + k, k, k + 4, to_pr) for k in range(4)]
    y_own = []
    for i, (src, dst) in enumerate(((s1, g1), (s2, g2), (s3, g3))):
        y_own.append(remote(src, dst.at[PREV - 1], y_send.at[i], y_recv.at[i], to_yn))
        y_own.append(remote(src, dst.at[NEXT - 1], y_send.at[3 + i], y_recv.at[3 + i], to_yp))
    y_far = [remote(g1.at[PREV - 1], g1.at[FAR - 1], y_send.at[6], y_recv.at[6], to_yn),
             remote(g2.at[PREV - 1], g2.at[FAR - 1], y_send.at[7], y_recv.at[7], to_yn),
             remote(g3.at[NEXT - 1], g3.at[FAR - 1], y_send.at[8], y_recv.at[8], to_yp)]

    def weights(e, slot):
        return [pltpu.make_async_copy(w1.at[e], w1b.at[slot], w_sem.at[slot, 0]),
                pltpu.make_async_copy(w3.at[e], w3b.at[slot], w_sem.at[slot, 1]),
                pltpu.make_async_copy(w2.at[e], w2b.at[slot], w_sem.at[slot, 2])]

    def push_rows(m, e):
        return remote(xr.at[e, pl.ds(4, 4)], rp.at[e], r_send.at[m, e], r_recv.at[m, e], to_pr)

    def first_far(m):
        return [remote(part.at[m, FAR, hi], rs1.at[m, 0], c_send.at[m, 4], c_recv.at[m, 4], to_xn),
                remote(part.at[m, FAR, lo], rs1.at[m, 1], c_send.at[m, 5], c_recv.at[m, 5], to_xp)]

    def near_own(m):
        return [remote(part.at[m, NEXT, lo], rfull.at[m, 0, lo], c_send.at[m, 0], c_recv.at[m, 0], to_xn),
                remote(part.at[m, PREV, hi], rfull.at[m, 1, hi], c_send.at[m, 1], c_recv.at[m, 1], to_xp)]

    def near_sum(m):
        return [remote(part.at[m, NEXT, hi], rfull.at[m, 0, hi], c_send.at[m, 2], c_recv.at[m, 2], to_xn),
                remote(part.at[m, PREV, lo], rfull.at[m, 1, lo], c_send.at[m, 3], c_recv.at[m, 3], to_xp)]

    tables = [pltpu.make_async_copy(src, dst, loc_sem.at[i]) for i, (src, dst) in enumerate((
        (ea, stage_e.at[0]), (sa, stage_s.at[0]), (ga, stage_g.at[0]),
        (eb, stage_e.at[1]), (sb, stage_s.at[1]), (gb, stage_g.at[1])))]
    local = [pltpu.make_async_copy(ta, tok.at[0, OWN], loc_sem.at[6]),
             pltpu.make_async_copy(tb, tok.at[1, OWN], loc_sem.at[7])]
    barrier = pltpu.get_barrier_semaphore()
    even_row = ty % 2 == 0
    for dev in (to_xn, to_xp, to_pr):
        pl.semaphore_signal(barrier, inc=1, device_id=dev, device_id_type=MESH)
    for cp in tables + local:
        cp.start()

    @pl.when(even_row)
    def _():
        pl.semaphore_wait(barrier, 3)
        for dev in (to_yn, to_yp):
            pl.semaphore_signal(barrier, inc=1, device_id=dev, device_id_type=MESH)

    @pl.when(jnp.logical_not(even_row))
    def _():
        pl.semaphore_wait(barrier, 5)
        for dev in (to_yn, to_yp):
            pl.semaphore_signal(y_ready, inc=1, device_id=dev, device_id_type=MESH)
    first = own_sends(0)
    for cp in first[:2] + [to_partner(0, OWN)]:
        cp.start()
    for cp in tables:
        cp.wait()
    for m in range(2):
        kept = stage_s[m] >= 0
        ids = jnp.where(kept, stage_e[m] * cap + stage_s[m], -1).astype(jnp.float32)
        routing[OWN, pl.ds(2 * m * top_k, top_k)] = ids
        routing[OWN, pl.ds((2 * m + 1) * top_k, top_k)] = jnp.where(kept, stage_g[m], 0.0)
    for cp in weights(0, 0) + [meta_next, meta_prev, meta_pair[OWN]] + first[2:]:
        cp.start()
    for cp in local:
        cp.wait()

    row_id = lax.broadcasted_iota(jnp.int32, (exp_rows, rows), 0).astype(jnp.float32)

    def placed(ids, base, values):
        shifted = row_id + (base * exp_rows).astype(jnp.float32)
        total = jnp.zeros((exp_rows, rows), jnp.float32)
        for j in range(top_k):
            total = jnp.where(shifted == ids[j:j + 1, :], 1.0 if values is None else values[j:j + 1, :], total)
        return total

    def row_ids(k, m):
        return routing[k, pl.ds(2 * m * top_k, top_k), :]

    def gates(k, m):
        return routing[k, pl.ds((2 * m + 1) * top_k, top_k), :]

    def pass_tokens():
        first[0].wait_recv()
        first[1].wait_recv()
        for cp in (meta_next, meta_prev):
            cp.wait_recv()
        for cp in forwards(0) + meta_far + own_sends(1) + [meta_pair[NEXT], meta_pair[PREV], to_partner(1, OWN)]:
            cp.start()

        @pl.when(even_row)
        def _():
            pl.semaphore_wait(y_ready, 2)
        for cp in y_own:
            cp.start()

    def arrivals(step):
        if step == 1:
            for cp in (meta_pair[OWN], to_partner(0, OWN)):
                cp.wait_recv()
        elif step == 2:
            first[2].wait_recv()
            first[3].wait_recv()
            to_partner(0, NEXT).start()
            to_partner(0, PREV).start()
        elif step in (3, 5):
            k = NEXT if step == 3 else PREV
            for cp in (meta_pair[k], to_partner(0, k)):
                cp.wait_recv()
        elif step == 6:
            for cp in meta_far:
                cp.wait_recv()
            meta_pair[FAR].start()
            for cp in forwards(0):
                cp.wait_recv()
            to_partner(0, FAR).start()
        elif step == 7:
            for cp in (meta_pair[FAR], to_partner(0, FAR)):
                cp.wait_recv()

    def pair_slot(block):
        return (block + 2) % 3 + block // 3

    def gather(m, first_step, last_step):
        def one(step, carry):
            if m == 0:
                for at in range(max(first_step, 1), last_step):
                    if at == 6:
                        continue
                    pl.when(step == at)(functools.partial(arrivals, at))
            block, other = step // 2, step % 2
            k = other * 4 + block
            place = placed(row_ids(k, m), ep, None).astype(jnp.bfloat16)
            got = jnp.dot(place, tok[m, k], preferred_element_type=jnp.float32).astype(jnp.bfloat16)
            at = (1 - other) * ((block + 1) % 4) + other * (4 + pair_slot(block))
            xr[:, at] = got.reshape(n_loc, cap, width)
            return carry
        lax.fori_loop(first_step, last_step, one, 0)

    def swiglu(x_rows, slot):
        proj_in = jnp.dot(x_rows, w1b[slot], preferred_element_type=jnp.float32)
        proj_gate = jnp.dot(x_rows, w3b[slot], preferred_element_type=jnp.float32)
        hidden = (jax.nn.silu(proj_in) * proj_gate).astype(jnp.bfloat16)
        return jnp.dot(hidden, w2b[slot], preferred_element_type=jnp.float32)

    def second_arrivals(step):
        sends = own_sends(1)
        if step == 0:
            sends[0].wait_recv()
            sends[1].wait_recv()
            for cp in forwards(1):
                cp.start()
        else:
            sends[2].wait_recv()
            sends[3].wait_recv()
            to_partner(1, NEXT).start()
            to_partner(1, PREV).start()

    early = n_loc // 2

    def run(e, slot, blocks):
        total = sum(b.size for b in blocks)
        x_rows = jnp.concatenate([xr[e, b].reshape(b.size * cap, width) for b in blocks], axis=0)
        res = swiglu(x_rows, slot).astype(jnp.bfloat16).reshape(total, cap, width)
        at = 0
        for b in blocks:
            xr[e, b] = res[at:at + b.size]
            at += b.size

    def stream(first, last, following, blocks, push, events=()):
        def one(e, carry):
            slot = e % 2
            for cp in weights(following(e), 1 - slot):
                cp.start()
            if push:
                @pl.when(e > 0)
                def _():
                    push_rows(0, e - 1).start()
            for cp in weights(e, slot):
                cp.wait()
            run(e, slot, blocks)
            for at, event in events:
                pl.when(e == at)(event)
            return carry
        lax.fori_loop(first, last, one, 0)

    def experts_first():
        own, far = [pl.ds(1, 1), pl.ds(6, 1)], [pl.ds(0, 1), pl.ds(7, 1)]
        near = [pl.ds(2, 4)]
        gather(0, 0, 2)
        stream(0, n_loc, lambda e: (e + 1) % n_loc, own, False, [(n_loc - 3, pass_tokens)])
        gather(0, 2, 6)
        stream(0, early, lambda e: (e + 1) % early, near, False, [(early - 2, functools.partial(arrivals, 6))])
        gather(0, 6, 8)
        stream(0, early, lambda e: e + 1, far, True, [(early - 1, functools.partial(second_arrivals, 0))])
        stream(early, n_loc, lambda e: (e + 1) % n_loc, [far[0]] + near + [far[1]], True)
        push_rows(0, n_loc - 1).start()

    def experts_second():
        def one(e, carry):
            slot = e % 2

            @pl.when(e < n_loc - 1)
            def _():
                for cp in weights(e + 1, 1 - slot):
                    cp.start()

            @pl.when(e > 0)
            def _():
                push_rows(1, e - 1).start()
            for cp in weights(e, slot):
                cp.wait()
            run(e, slot, [pl.ds(0, 8)])

            @pl.when(e == early)
            def _():
                for cp in y_own:
                    cp.wait_recv()
                for cp in y_far:
                    cp.start()
            return carry
        lax.fori_loop(0, n_loc, one, 0)
        push_rows(1, n_loc - 1).start()

    def combine(m):
        chunks = [pl.ds(n * 256, 256) for n in range(width // 256)]

        def weigh(gate_rows, rows_of, cols):
            acc = jnp.dot(gate_rows, rows_of(cols).reshape(exp_rows, 256), preferred_element_type=jnp.float32)
            return acc[0:rows] + acc[rows:2 * rows] + acc[2 * rows:3 * rows]

        def one(step, carry):
            i = 3 - step
            ids = row_ids(i, m)
            vals = gates(i, m)
            mine = jnp.concatenate(split_three(placed(ids, ep, vals).T), axis=0)
            other = jnp.concatenate(split_three(placed(ids, partner, vals).T), axis=0)
            at = (i + 1) % 4
            for cols in chunks:
                part[m, i, :, cols] = weigh(mine, lambda c: xr[:, at, :, c], cols)

            @pl.when(step == 0)
            def _():
                for e in range(n_loc):
                    push_rows(m, e).wait_recv()
            for cols in chunks:
                part[m, i, :, cols] += weigh(other, lambda c: rp[:, pair_slot(i), :, c], cols)

            @pl.when(step == 0)
            def _():
                for cp in first_far(m):
                    cp.start()

            @pl.when(step == 1)
            def _():
                near_own(m)[1].start()
                if m == 0:
                    second_arrivals(1)

            @pl.when(step == 2)
            def _():
                near_own(m)[0].start()
            return carry
        lax.fori_loop(0, 4, one, 0)

    def pass_on(m):
        incoming = first_far(m)
        sends = near_sum(m)
        incoming[0].wait_recv()
        part[m, NEXT, hi] = part[m, NEXT, hi] + rs1[m, 0]
        sends[0].start()
        incoming[1].wait_recv()
        part[m, PREV, lo] = part[m, PREV, lo] + rs1[m, 1]
        sends[1].start()

    def finish(m, out):
        for cp in near_own(m) + near_sum(m):
            cp.wait_recv()
        total = part[m, OWN] + tok[m, OWN].astype(jnp.float32) + rfull[m, 0] + rfull[m, 1]
        out[...] = total.astype(jnp.bfloat16)

    experts_first()
    combine(0)
    for cp in forwards(1):
        cp.wait_recv()
    to_partner(1, FAR).start()
    pl.semaphore_signal(free_sem, inc=1, device_id=to_pr, device_id_type=MESH)
    for k in range(4):
        to_partner(1, k).wait_recv()
    for e in range(n_loc):
        push_rows(0, e).wait_send()
    gather(1, 0, 8)
    pl.semaphore_wait(free_sem, 1)
    experts_second()
    pass_on(0)
    combine(1)
    for cp in y_far:
        cp.wait_recv()
    shared = []
    for slot, pair in enumerate((((s1, s3, s2), NEXT), (None, FAR))):
        srcs = [pair[0] or (g1.at[PREV - 1], g3.at[PREV - 1], g2.at[PREV - 1]), (g1.at[pair[1] - 1], g3.at[pair[1] - 1], g2.at[pair[1] - 1])]
        for p, (a1, a3, a2) in enumerate(srcs):
            part_of = pl.ds(p * sh, sh)
            shared.append(pltpu.make_async_copy(a1, w1b.at[slot, :, part_of], w_sem.at[slot, 3 + p]))
            shared.append(pltpu.make_async_copy(a3, w3b.at[slot, :, part_of], w_sem.at[slot, 5 + p]))
            shared.append(pltpu.make_async_copy(a2, w2b.at[slot, part_of, :], w_sem.at[slot, 7 + p]))
    for cp in shared:
        cp.start()
    for cp in shared:
        cp.wait()

    def shared_one(i, carry):
        m = i // 2
        part[m, OWN] = part[m, OWN] + swiglu(tok[m, OWN], i % 2)
        return carry
    lax.fori_loop(0, 4, shared_one, 0)

    finish(0, out_a)
    pass_on(1)
    finish(1, out_b)
    for m in range(2):
        for k in range(4):
            to_partner(m, k).wait_send()
        for cp in own_sends(m) + forwards(m) + first_far(m) + near_own(m) + near_sum(m):
            cp.wait_send()
    for e in range(n_loc):
        push_rows(1, e).wait_send()
    for cp in [meta_next, meta_prev] + meta_far + meta_pair + y_own + y_far:
        cp.wait_send()


def solution(mesh):
    ep_size = mesh.shape['ep']
    tp_size = mesh.shape['tp']
    tok_spec = P(('data', 'ep', 'tp'), None)
    in_specs = (tok_spec,) * 8 + (P(None, 'tp'), P(None, 'tp'), P('tp', None), P('ep', None, None), P('ep', None, None), P('ep', None, None))

    def layer_local(tokens_a, tokens_b, experts_a, experts_b, gates_a, gates_b, slots_a, slots_b, shared_w1, shared_w3, shared_w2, routed_w1, routed_w3, routed_w2):
        rows, width = tokens_a.shape
        top_k = experts_a.shape[1]
        n_loc, _, ff = routed_w1.shape
        sh = shared_w1.shape[1]
        cap = capacity_rows(rows, top_k, n_loc * ep_size)
        half = rows // 2
        tables = [a.T for a in (experts_a, experts_b, gates_a, gates_b, slots_a, slots_b)]
        bf, f32 = jnp.bfloat16, jnp.float32
        dma = pltpu.SemaphoreType.DMA
        any_spec = pl.BlockSpec(memory_space=pl.ANY)
        vmem_spec = pl.BlockSpec(memory_space=pltpu.VMEM)
        outs = pl.pallas_call(
            functools.partial(layer_kernel, (top_k, ep_size, tp_size, cap)),
            out_shape=(pltpu.VMEM((rows, width), bf), pltpu.VMEM((rows, width), bf),
                       jax.ShapeDtypeStruct((3, width, sh), bf), jax.ShapeDtypeStruct((3, width, sh), bf),
                       jax.ShapeDtypeStruct((3, sh, width), bf)),
            in_specs=[any_spec] * 14,
            out_specs=[vmem_spec] * 2 + [any_spec] * 3,
            scratch_shapes=[
                pltpu.VMEM((2, 8, rows, width), bf),
                pltpu.VMEM((8, 4 * top_k, rows), f32),
                pltpu.VMEM((2, top_k, rows), jnp.int32),
                pltpu.VMEM((2, top_k, rows), jnp.int32),
                pltpu.VMEM((2, top_k, rows), f32),
                pltpu.VMEM((n_loc, 8, cap, width), bf),
                pltpu.VMEM((n_loc, 4, cap, width), bf),
                pltpu.VMEM((2, width, ff), bf),
                pltpu.VMEM((2, width, ff), bf),
                pltpu.VMEM((2, ff, width), bf),
                pltpu.VMEM((2, 4, rows, width), f32),
                pltpu.VMEM((2, 2, half, width), f32),
                pltpu.VMEM((2, 2, rows, width), f32),
                dma((8,)), dma((2, 9)), dma((2, 6)), dma((2, 6)), dma((2, 4)), dma((2, 4)), dma((8,)), dma((8,)),
                dma((9,)), dma((9,)), dma((2, n_loc)), dma((2, n_loc)), dma((2, 6)), dma((2, 6)),
                pltpu.SemaphoreType.REGULAR, pltpu.SemaphoreType.REGULAR,
            ],
            compiler_params=pltpu.CompilerParams(collective_id=0, has_side_effects=True, vmem_limit_bytes=VMEM_BYTES),
        )(*tables, tokens_a, tokens_b, shared_w1, shared_w3, shared_w2, routed_w1, routed_w3, routed_w2)
        return outs[0], outs[1]

    return jax.shard_map(layer_local, mesh=mesh, in_specs=in_specs, out_specs=(tok_spec, tok_spec), check_vma=False)
```

```python
import functools

import jax
import jax.numpy as jnp
from jax import lax
from jax.experimental import pallas as pl
from jax.experimental.pallas import tpu as pltpu
from jax.sharding import PartitionSpec as P

MESH = pl.DeviceIdType.MESH
VMEM_BYTES = 65000000
CORES = 2
OWN, NEXT, PREV, FAR = 0, 1, 2, 3


def capacity_rows(tok_local, top_k, num_experts):
    return max(4, (2 * tok_local * top_k) // num_experts)


def split_three(value):
    hi = value.astype(jnp.bfloat16)
    rest = value - hi.astype(jnp.float32)
    mid = rest.astype(jnp.bfloat16)
    low = (rest - mid.astype(jnp.float32)).astype(jnp.bfloat16)
    return hi, mid, low


def layer_kernel(cfg, ea, eb, ga, gb, sa, sb, ta, tb, s1, s3, s2, w1, w3, w2, out_a, out_b, g1, g3, g2,
                 tok, routing, stage_e, stage_s, stage_g, xr, rp, w1b, w3b, w2b, part, rs1, rfull,
                 loc_sem, w_sem, tx_send, tx_recv, tp_send, tp_recv, mt_send, mt_recv,
                 y_send, y_recv, r_send, r_recv, c_send, c_recv, free_sem, y_ready):
    top_k, ep_size, tp_size, cap = cfg
    n_loc = w1.shape[0]
    ff = w1.shape[2]
    sh = s1.shape[1]
    rows, width = ta.shape
    half = rows // 2
    exp_rows = n_loc * cap
    nx = ep_size // CORES
    ep = lax.axis_index('ep')
    ty = lax.axis_index('tp')
    core = ep % CORES
    chip = ep // CORES
    partner = chip * CORES + (1 - core)
    x_next = ((chip + 1) % nx) * CORES + core
    x_prev = ((chip + nx - 1) % nx) * CORES + core
    y_next = (ty + 1) % tp_size
    y_prev = (ty + tp_size - 1) % tp_size
    to_xn, to_xp, to_pr = {'ep': x_next}, {'ep': x_prev}, {'ep': partner}
    to_yn, to_yp = {'tp': y_next}, {'tp': y_prev}
    lo, hi = pl.ds(0, half), pl.ds(half, half)

    def remote(src, dst, ssem, rsem, dev):
        return pltpu.make_async_remote_copy(src_ref=src, dst_ref=dst, send_sem=ssem, recv_sem=rsem,
                                            device_id=dev, device_id_type=MESH)

    def own_sends(m):
        mine = (ta, tb)[m]
        return [remote(mine.at[lo], tok.at[m, PREV, lo], tx_send.at[m, 0], tx_recv.at[m, 0], to_xn),
                remote(mine.at[hi], tok.at[m, NEXT, hi], tx_send.at[m, 3], tx_recv.at[m, 3], to_xp),
                remote(mine.at[hi], tok.at[m, PREV, hi], tx_send.at[m, 1], tx_recv.at[m, 1], to_xn),
                remote(mine.at[lo], tok.at[m, NEXT, lo], tx_send.at[m, 2], tx_recv.at[m, 2], to_xp)]

    def forwards(m):
        return [remote(tok.at[m, PREV, lo], tok.at[m, FAR, lo], tx_send.at[m, 4], tx_recv.at[m, 4], to_xn),
                remote(tok.at[m, NEXT, hi], tok.at[m, FAR, hi], tx_send.at[m, 5], tx_recv.at[m, 5], to_xp)]

    def to_partner(m, k):
        return remote((ta, tb)[m] if k == OWN else tok.at[m, k], tok.at[m, k + 4], tp_send.at[m, k], tp_recv.at[m, k], to_pr)

    def meta(i, src, dst, dev, lines=pl.ds(0, 4 * top_k)):
        return remote(routing.at[src, lines], routing.at[dst, lines], mt_send.at[i], mt_recv.at[i], dev)

    far_cut = (4 * top_k * 2 // 3) // 8 * 8
    meta_next = meta(0, OWN, PREV, to_xn)
    meta_prev = meta(1, OWN, NEXT, to_xp)
    meta_far = [meta(2, PREV, FAR, to_xn, pl.ds(0, far_cut)),
                meta(3, NEXT, FAR, to_xp, pl.ds(far_cut, 4 * top_k - far_cut))]
    meta_pair = [meta(4 + k, k, k + 4, to_pr) for k in range(4)]
    y_own = []
    for i, (src, dst) in enumerate(((s1, g1), (s2, g2), (s3, g3))):
        y_own.append(remote(src, dst.at[PREV - 1], y_send.at[i], y_recv.at[i], to_yn))
        y_own.append(remote(src, dst.at[NEXT - 1], y_send.at[3 + i], y_recv.at[3 + i], to_yp))
    y_far = [remote(g1.at[PREV - 1], g1.at[FAR - 1], y_send.at[6], y_recv.at[6], to_yn),
             remote(g2.at[PREV - 1], g2.at[FAR - 1], y_send.at[7], y_recv.at[7], to_yn),
             remote(g3.at[NEXT - 1], g3.at[FAR - 1], y_send.at[8], y_recv.at[8], to_yp)]

    def weights(e, slot):
        return [pltpu.make_async_copy(w1.at[e], w1b.at[slot], w_sem.at[slot, 0]),
                pltpu.make_async_copy(w3.at[e], w3b.at[slot], w_sem.at[slot, 1]),
                pltpu.make_async_copy(w2.at[e], w2b.at[slot], w_sem.at[slot, 2])]

    def push_rows(m, e):
        return remote(xr.at[e, pl.ds(4, 4)], rp.at[e], r_send.at[m, e], r_recv.at[m, e], to_pr)

    def first_far(m):
        return [remote(part.at[m, FAR, hi], rs1.at[m, 0], c_send.at[m, 4], c_recv.at[m, 4], to_xn),
                remote(part.at[m, FAR, lo], rs1.at[m, 1], c_send.at[m, 5], c_recv.at[m, 5], to_xp)]

    def near_own(m):
        return [remote(part.at[m, NEXT, lo], rfull.at[m, 0, lo], c_send.at[m, 0], c_recv.at[m, 0], to_xn),
                remote(part.at[m, PREV, hi], rfull.at[m, 1, hi], c_send.at[m, 1], c_recv.at[m, 1], to_xp)]

    def near_sum(m):
        return [remote(part.at[m, NEXT, hi], rfull.at[m, 0, hi], c_send.at[m, 2], c_recv.at[m, 2], to_xn),
                remote(part.at[m, PREV, lo], rfull.at[m, 1, lo], c_send.at[m, 3], c_recv.at[m, 3], to_xp)]

    tables = [pltpu.make_async_copy(src, dst, loc_sem.at[i]) for i, (src, dst) in enumerate((
        (ea, stage_e.at[0]), (sa, stage_s.at[0]), (ga, stage_g.at[0]),
        (eb, stage_e.at[1]), (sb, stage_s.at[1]), (gb, stage_g.at[1])))]
    local = [pltpu.make_async_copy(ta, tok.at[0, OWN], loc_sem.at[6]),
             pltpu.make_async_copy(tb, tok.at[1, OWN], loc_sem.at[7])]
    barrier = pltpu.get_barrier_semaphore()
    is_first, is_last = ty == 0, ty == tp_size - 1

    def greet(sem, dev):
        pl.semaphore_signal(sem, inc=1, device_id=dev, device_id_type=MESH)

    for dev in (to_xn, to_xp, to_pr):
        greet(barrier, dev)
    for cp in tables + local:
        cp.start()

    @pl.when(is_first)
    def _():
        pl.semaphore_wait(barrier, 3)
        greet(barrier, to_yn)
        greet(barrier, to_yp)

    @pl.when(jnp.logical_not(jnp.logical_or(is_first, is_last)))
    def _():
        pl.semaphore_wait(barrier, 4)
        greet(barrier, to_yn)
        greet(y_ready, to_yp)

    @pl.when(is_last)
    def _():
        pl.semaphore_wait(barrier, 5)
        greet(y_ready, to_yn)
        greet(y_ready, to_yp)
    first = own_sends(0)
    for cp in first[:2] + [to_partner(0, OWN)]:
        cp.start()
    for cp in tables:
        cp.wait()
    for m in range(2):
        kept = stage_s[m] >= 0
        ids = jnp.where(kept, stage_e[m] * cap + stage_s[m], -1).astype(jnp.float32)
        routing[OWN, pl.ds(2 * m * top_k, top_k)] = ids
        routing[OWN, pl.ds((2 * m + 1) * top_k, top_k)] = jnp.where(kept, stage_g[m], 0.0)
    for cp in weights(0, 0) + [meta_next, meta_prev, meta_pair[OWN]] + first[2:]:
        cp.start()
    for cp in local:
        cp.wait()

    row_id = lax.broadcasted_iota(jnp.int32, (exp_rows, rows), 0).astype(jnp.float32)

    def placed(ids, base, values):
        shifted = row_id + (base * exp_rows).astype(jnp.float32)
        total = jnp.zeros((exp_rows, rows), jnp.float32)
        for j in range(top_k):
            total = jnp.where(shifted == ids[j:j + 1, :], 1.0 if values is None else values[j:j + 1, :], total)
        return total

    def row_ids(k, m):
        return routing[k, pl.ds(2 * m * top_k, top_k), :]

    def gates(k, m):
        return routing[k, pl.ds((2 * m + 1) * top_k, top_k), :]

    def pass_tokens():
        first[0].wait_recv()
        first[1].wait_recv()
        for cp in (meta_next, meta_prev):
            cp.wait_recv()
        for cp in forwards(0) + meta_far + own_sends(1) + [meta_pair[NEXT], meta_pair[PREV], to_partner(1, OWN)]:
            cp.start()

        @pl.when(is_first)
        def _():
            pl.semaphore_wait(y_ready, 2)

        @pl.when(jnp.logical_not(jnp.logical_or(is_first, is_last)))
        def _():
            pl.semaphore_wait(y_ready, 1)
        for cp in y_own:
            cp.start()

    def arrivals(step):
        if step == 1:
            for cp in (meta_pair[OWN], to_partner(0, OWN)):
                cp.wait_recv()
        elif step == 2:
            first[2].wait_recv()
            first[3].wait_recv()
            to_partner(0, NEXT).start()
            to_partner(0, PREV).start()
        elif step in (3, 5):
            k = NEXT if step == 3 else PREV
            for cp in (meta_pair[k], to_partner(0, k)):
                cp.wait_recv()
        elif step == 6:
            for cp in meta_far:
                cp.wait_recv()
            meta_pair[FAR].start()
            for cp in forwards(0):
                cp.wait_recv()
            to_partner(0, FAR).start()
        elif step == 7:
            for cp in (meta_pair[FAR], to_partner(0, FAR)):
                cp.wait_recv()

    def pair_slot(block):
        return (block + 2) % 3 + block // 3

    def gather(m, first_step, last_step):
        def one(step, carry):
            if m == 0:
                for at in range(max(first_step, 1), last_step):
                    if at == 6:
                        continue
                    pl.when(step == at)(functools.partial(arrivals, at))
            block, other = step // 2, step % 2
            k = other * 4 + block
            place = placed(row_ids(k, m), ep, None).astype(jnp.bfloat16)
            got = jnp.dot(place, tok[m, k], preferred_element_type=jnp.float32).astype(jnp.bfloat16)
            at = (1 - other) * ((block + 1) % 4) + other * (4 + pair_slot(block))
            xr[:, at] = got.reshape(n_loc, cap, width)
            return carry
        lax.fori_loop(first_step, last_step, one, 0)

    def swiglu(x_rows, slot):
        proj_in = jnp.dot(x_rows, w1b[slot], preferred_element_type=jnp.float32)
        proj_gate = jnp.dot(x_rows, w3b[slot], preferred_element_type=jnp.float32)
        hidden = (jax.nn.silu(proj_in) * proj_gate).astype(jnp.bfloat16)
        return jnp.dot(hidden, w2b[slot], preferred_element_type=jnp.float32)

    def second_arrivals(step):
        sends = own_sends(1)
        if step == 0:
            sends[0].wait_recv()
            sends[1].wait_recv()
            for cp in forwards(1):
                cp.start()
        else:
            sends[2].wait_recv()
            sends[3].wait_recv()
            to_partner(1, NEXT).start()
            to_partner(1, PREV).start()

    early = n_loc // 2

    def run(e, slot, blocks):
        total = sum(b.size for b in blocks)
        x_rows = jnp.concatenate([xr[e, b].reshape(b.size * cap, width) for b in blocks], axis=0)
        res = swiglu(x_rows, slot).astype(jnp.bfloat16).reshape(total, cap, width)
        at = 0
        for b in blocks:
            xr[e, b] = res[at:at + b.size]
            at += b.size

    def stream(first, last, following, blocks, push, events=()):
        def one(e, carry):
            slot = e % 2
            for cp in weights(following(e), 1 - slot):
                cp.start()
            if push:
                @pl.when(e > 0)
                def _():
                    push_rows(0, e - 1).start()
            for cp in weights(e, slot):
                cp.wait()
            run(e, slot, blocks)
            for at, event in events:
                pl.when(e == at)(event)
            return carry
        lax.fori_loop(first, last, one, 0)

    def experts_first():
        own, far = [pl.ds(1, 1), pl.ds(6, 1)], [pl.ds(0, 1), pl.ds(7, 1)]
        near = [pl.ds(2, 4)]
        gather(0, 0, 2)
        stream(0, n_loc, lambda e: (e + 1) % n_loc, own, False, [(n_loc - 3, pass_tokens)])
        gather(0, 2, 6)
        stream(0, early, lambda e: (e + 1) % early, near, False, [(early - 2, functools.partial(arrivals, 6))])
        gather(0, 6, 8)
        stream(0, early, lambda e: e + 1, far, True, [(early - 1, functools.partial(second_arrivals, 0))])
        stream(early, n_loc, lambda e: (e + 1) % n_loc, [far[0]] + near + [far[1]], True)
        push_rows(0, n_loc - 1).start()

    def experts_second():
        def one(e, carry):
            slot = e % 2

            @pl.when(e < n_loc - 1)
            def _():
                for cp in weights(e + 1, 1 - slot):
                    cp.start()

            @pl.when(e > 0)
            def _():
                push_rows(1, e - 1).start()
            for cp in weights(e, slot):
                cp.wait()
            run(e, slot, [pl.ds(0, 8)])

            @pl.when(e == early)
            def _():
                for cp in y_own:
                    cp.wait_recv()
                for cp in y_far:
                    cp.start()
            return carry
        lax.fori_loop(0, n_loc, one, 0)
        push_rows(1, n_loc - 1).start()

    def combine(m):
        chunks = [pl.ds(n * 256, 256) for n in range(width // 256)]

        def weigh(gate_rows, rows_of, cols):
            acc = jnp.dot(gate_rows, rows_of(cols).reshape(exp_rows, 256), preferred_element_type=jnp.float32)
            return acc[0:rows] + acc[rows:2 * rows] + acc[2 * rows:3 * rows]

        def one(step, carry):
            i = 3 - step
            ids = row_ids(i, m)
            vals = gates(i, m)
            mine = jnp.concatenate(split_three(placed(ids, ep, vals).T), axis=0)
            other = jnp.concatenate(split_three(placed(ids, partner, vals).T), axis=0)
            at = (i + 1) % 4
            for cols in chunks:
                part[m, i, :, cols] = weigh(mine, lambda c: xr[:, at, :, c], cols)

            @pl.when(step == 0)
            def _():
                for e in range(n_loc):
                    push_rows(m, e).wait_recv()
            for cols in chunks:
                part[m, i, :, cols] += weigh(other, lambda c: rp[:, pair_slot(i), :, c], cols)

            @pl.when(step == 0)
            def _():
                for cp in first_far(m):
                    cp.start()

            @pl.when(step == 1)
            def _():
                near_own(m)[1].start()
                if m == 0:
                    second_arrivals(1)

            @pl.when(step == 2)
            def _():
                near_own(m)[0].start()
            return carry
        lax.fori_loop(0, 4, one, 0)

    def pass_on(m):
        incoming = first_far(m)
        sends = near_sum(m)
        incoming[0].wait_recv()
        part[m, NEXT, hi] = part[m, NEXT, hi] + rs1[m, 0]
        sends[0].start()
        incoming[1].wait_recv()
        part[m, PREV, lo] = part[m, PREV, lo] + rs1[m, 1]
        sends[1].start()

    def near_ready(m):
        for cp in near_own(m):
            cp.wait_recv()
        part[m, OWN, lo] += tok[m, OWN, lo].astype(jnp.float32) + rfull[m, 0, lo]
        part[m, OWN, hi] += tok[m, OWN, hi].astype(jnp.float32) + rfull[m, 1, hi]

    def finish(m, out):
        sums = near_sum(m)
        sums[0].wait_recv()
        out[hi] = (part[m, OWN, hi] + rfull[m, 0, hi]).astype(jnp.bfloat16)
        sums[1].wait_recv()
        out[lo] = (part[m, OWN, lo] + rfull[m, 1, lo]).astype(jnp.bfloat16)

    experts_first()
    combine(0)
    for cp in forwards(1):
        cp.wait_recv()
    to_partner(1, FAR).start()
    pl.semaphore_signal(free_sem, inc=1, device_id=to_pr, device_id_type=MESH)
    for k in range(4):
        to_partner(1, k).wait_recv()
    for e in range(n_loc):
        push_rows(0, e).wait_send()
    gather(1, 0, 8)
    pl.semaphore_wait(free_sem, 1)
    experts_second()
    pass_on(0)
    combine(1)
    for cp in y_far:
        cp.wait_recv()
    shared = []
    for slot, pair in enumerate((((s1, s3, s2), NEXT), (None, FAR))):
        srcs = [pair[0] or (g1.at[PREV - 1], g3.at[PREV - 1], g2.at[PREV - 1]), (g1.at[pair[1] - 1], g3.at[pair[1] - 1], g2.at[pair[1] - 1])]
        for p, (a1, a3, a2) in enumerate(srcs):
            part_of = pl.ds(p * sh, sh)
            shared.append(pltpu.make_async_copy(a1, w1b.at[slot, :, part_of], w_sem.at[slot, 3 + p]))
            shared.append(pltpu.make_async_copy(a3, w3b.at[slot, :, part_of], w_sem.at[slot, 5 + p]))
            shared.append(pltpu.make_async_copy(a2, w2b.at[slot, part_of, :], w_sem.at[slot, 7 + p]))
    for cp in shared:
        cp.start()
    for cp in shared:
        cp.wait()

    def shared_one(i, carry):
        m = i // 2
        part[m, OWN] = part[m, OWN] + swiglu(tok[m, OWN], i % 2)
        return carry
    lax.fori_loop(0, 4, shared_one, 0)

    near_ready(0)
    finish(0, out_a)
    pass_on(1)
    near_ready(1)
    finish(1, out_b)
    for m in range(2):
        for k in range(4):
            to_partner(m, k).wait_send()
        for cp in own_sends(m) + forwards(m) + first_far(m) + near_own(m) + near_sum(m):
            cp.wait_send()
    for e in range(n_loc):
        push_rows(1, e).wait_send()
    for cp in [meta_next, meta_prev] + meta_far + meta_pair + y_own + y_far:
        cp.wait_send()


def place_kernel(a, b, out_a, out_b, sem):
    copies = [pltpu.make_async_copy(a, out_a, sem.at[0]), pltpu.make_async_copy(b, out_b, sem.at[1])]
    for cp in copies:
        cp.start()
    for cp in copies:
        cp.wait()


def solution(mesh):
    ep_size = mesh.shape['ep']
    tp_size = mesh.shape['tp']
    tok_spec = P(('data', 'ep', 'tp'), None)
    in_specs = (tok_spec,) * 8 + (P(None, 'tp'), P(None, 'tp'), P('tp', None), P('ep', None, None), P('ep', None, None), P('ep', None, None))

    def layer_local(tokens_a, tokens_b, experts_a, experts_b, gates_a, gates_b, slots_a, slots_b, shared_w1, shared_w3, shared_w2, routed_w1, routed_w3, routed_w2):
        rows, width = tokens_a.shape
        top_k = experts_a.shape[1]
        n_loc, _, ff = routed_w1.shape
        sh = shared_w1.shape[1]
        cap = capacity_rows(rows, top_k, n_loc * ep_size)
        half = rows // 2
        tables = [a.T for a in (experts_a, experts_b, gates_a, gates_b, slots_a, slots_b)]
        bf, f32 = jnp.bfloat16, jnp.float32
        dma = pltpu.SemaphoreType.DMA
        any_spec = pl.BlockSpec(memory_space=pl.ANY)
        vmem_spec = pl.BlockSpec(memory_space=pltpu.VMEM)
        outs = pl.pallas_call(
            functools.partial(layer_kernel, (top_k, ep_size, tp_size, cap)),
            out_shape=(pltpu.VMEM((rows, width), bf), pltpu.VMEM((rows, width), bf),
                       jax.ShapeDtypeStruct((3, width, sh), bf), jax.ShapeDtypeStruct((3, width, sh), bf),
                       jax.ShapeDtypeStruct((3, sh, width), bf)),
            in_specs=[any_spec] * 14,
            out_specs=[vmem_spec] * 2 + [any_spec] * 3,
            scratch_shapes=[
                pltpu.VMEM((2, 8, rows, width), bf),
                pltpu.VMEM((8, 4 * top_k, rows), f32),
                pltpu.VMEM((2, top_k, rows), jnp.int32),
                pltpu.VMEM((2, top_k, rows), jnp.int32),
                pltpu.VMEM((2, top_k, rows), f32),
                pltpu.VMEM((n_loc, 8, cap, width), bf),
                pltpu.VMEM((n_loc, 4, cap, width), bf),
                pltpu.VMEM((2, width, ff), bf),
                pltpu.VMEM((2, width, ff), bf),
                pltpu.VMEM((2, ff, width), bf),
                pltpu.VMEM((2, 4, rows, width), f32),
                pltpu.VMEM((2, 2, half, width), f32),
                pltpu.VMEM((2, 2, rows, width), f32),
                dma((8,)), dma((2, 9)), dma((2, 6)), dma((2, 6)), dma((2, 4)), dma((2, 4)), dma((8,)), dma((8,)),
                dma((9,)), dma((9,)), dma((2, n_loc)), dma((2, n_loc)), dma((2, 6)), dma((2, 6)),
                pltpu.SemaphoreType.REGULAR, pltpu.SemaphoreType.REGULAR,
            ],
            compiler_params=pltpu.CompilerParams(collective_id=0, has_side_effects=True, vmem_limit_bytes=VMEM_BYTES),
        )(*tables, tokens_a, tokens_b, shared_w1, shared_w3, shared_w2, routed_w1, routed_w3, routed_w2)
        held = outs[:2]
        return pl.pallas_call(
            place_kernel,
            out_shape=(jax.ShapeDtypeStruct((rows, width), bf),) * 2,
            in_specs=[vmem_spec] * 2,
            out_specs=[any_spec] * 2,
            scratch_shapes=[dma((2,))],
            compiler_params=pltpu.CompilerParams(vmem_limit_bytes=1 << 20),
        )(*held)

    return jax.shard_map(layer_local, mesh=mesh, in_specs=in_specs, out_specs=(tok_spec, tok_spec), check_vma=False)
```

```python
import functools

import jax
import jax.numpy as jnp
from jax import lax
from jax.experimental import pallas as pl
from jax.experimental.pallas import tpu as pltpu
from jax.sharding import PartitionSpec as P

MESH = pl.DeviceIdType.MESH
VMEM_BYTES = 65000000
BF16_TOP = float(jnp.finfo(jnp.bfloat16).max)
CORES = 2
OWN, NEXT, PREV, FAR = 0, 1, 2, 3


def capacity_rows(tok_local, top_k, num_experts):
    return max(4, (2 * tok_local * top_k) // num_experts)


def split_three(value):
    hi = jnp.minimum(value, BF16_TOP).astype(jnp.bfloat16)
    rest = value - hi.astype(jnp.float32)
    mid = rest.astype(jnp.bfloat16)
    low = (rest - mid.astype(jnp.float32)).astype(jnp.bfloat16)
    return hi, mid, low


def layer_kernel(cfg, ea, eb, ga, gb, sa, sb, ta, tb, s1, s3, s2, w1, w3, w2, out_a, out_b, g1, g3, g2,
                 tok, routing, stage_e, stage_s, stage_g, xr, rp, w1b, w3b, w2b, part, rs1, rfull,
                 loc_sem, w_sem, tx_send, tx_recv, tp_send, tp_recv, mt_send, mt_recv,
                 y_send, y_recv, r_send, r_recv, c_send, c_recv, free_sem, y_ready):
    top_k, ep_size, tp_size, cap = cfg
    n_loc = w1.shape[0]
    ff = w1.shape[2]
    sh = s1.shape[1]
    rows, width = ta.shape
    half = rows // 2
    exp_rows = n_loc * cap
    nx = ep_size // CORES
    ep = lax.axis_index('ep')
    ty = lax.axis_index('tp')
    core = ep % CORES
    chip = ep // CORES
    partner = chip * CORES + (1 - core)
    x_next = ((chip + 1) % nx) * CORES + core
    x_prev = ((chip + nx - 1) % nx) * CORES + core
    y_next = (ty + 1) % tp_size
    y_prev = (ty + tp_size - 1) % tp_size
    to_xn, to_xp, to_pr = {'ep': x_next}, {'ep': x_prev}, {'ep': partner}
    to_yn, to_yp = {'tp': y_next}, {'tp': y_prev}
    lo, hi = pl.ds(0, half), pl.ds(half, half)

    def remote(src, dst, ssem, rsem, dev):
        return pltpu.make_async_remote_copy(src_ref=src, dst_ref=dst, send_sem=ssem, recv_sem=rsem,
                                            device_id=dev, device_id_type=MESH)

    def own_sends(m):
        mine = (ta, tb)[m]
        return [remote(mine.at[lo], tok.at[m, PREV, lo], tx_send.at[m, 0], tx_recv.at[m, 0], to_xn),
                remote(mine.at[hi], tok.at[m, NEXT, hi], tx_send.at[m, 3], tx_recv.at[m, 3], to_xp),
                remote(mine.at[hi], tok.at[m, PREV, hi], tx_send.at[m, 1], tx_recv.at[m, 1], to_xn),
                remote(mine.at[lo], tok.at[m, NEXT, lo], tx_send.at[m, 2], tx_recv.at[m, 2], to_xp)]

    def forwards(m):
        return [remote(tok.at[m, PREV, lo], tok.at[m, FAR, lo], tx_send.at[m, 4], tx_recv.at[m, 4], to_xn),
                remote(tok.at[m, NEXT, hi], tok.at[m, FAR, hi], tx_send.at[m, 5], tx_recv.at[m, 5], to_xp)]

    def to_partner(m, k):
        return remote((ta, tb)[m] if k == OWN else tok.at[m, k], tok.at[m, k + 4], tp_send.at[m, k], tp_recv.at[m, k], to_pr)

    def meta(i, src, dst, dev, lines=pl.ds(0, 4 * top_k)):
        return remote(routing.at[src, lines], routing.at[dst, lines], mt_send.at[i], mt_recv.at[i], dev)

    far_cut = (4 * top_k * 2 // 3) // 8 * 8
    meta_next = meta(0, OWN, PREV, to_xn)
    meta_prev = meta(1, OWN, NEXT, to_xp)
    meta_far = [meta(2, PREV, FAR, to_xn, pl.ds(0, far_cut)),
                meta(3, NEXT, FAR, to_xp, pl.ds(far_cut, 4 * top_k - far_cut))]
    meta_pair = [meta(4 + k, k, k + 4, to_pr) for k in range(4)]
    y_own = []
    for i, (src, dst) in enumerate(((s1, g1), (s2, g2), (s3, g3))):
        y_own.append(remote(src, dst.at[PREV - 1], y_send.at[i], y_recv.at[i], to_yn))
        y_own.append(remote(src, dst.at[NEXT - 1], y_send.at[3 + i], y_recv.at[3 + i], to_yp))
    y_far = [remote(g1.at[PREV - 1], g1.at[FAR - 1], y_send.at[6], y_recv.at[6], to_yn),
             remote(g2.at[PREV - 1], g2.at[FAR - 1], y_send.at[7], y_recv.at[7], to_yn),
             remote(g3.at[NEXT - 1], g3.at[FAR - 1], y_send.at[8], y_recv.at[8], to_yp)]

    def weights(e, slot):
        return [pltpu.make_async_copy(w1.at[e], w1b.at[slot], w_sem.at[slot, 0]),
                pltpu.make_async_copy(w3.at[e], w3b.at[slot], w_sem.at[slot, 1]),
                pltpu.make_async_copy(w2.at[e], w2b.at[slot], w_sem.at[slot, 2])]

    def push_rows(m, e):
        return remote(xr.at[e, pl.ds(4, 4)], rp.at[e], r_send.at[m, e], r_recv.at[m, e], to_pr)

    def first_far(m):
        return [remote(part.at[m, FAR, hi], rs1.at[m, 0], c_send.at[m, 4], c_recv.at[m, 4], to_xn),
                remote(part.at[m, FAR, lo], rs1.at[m, 1], c_send.at[m, 5], c_recv.at[m, 5], to_xp)]

    def near_own(m):
        return [remote(part.at[m, NEXT, lo], rfull.at[m, 0, lo], c_send.at[m, 0], c_recv.at[m, 0], to_xn),
                remote(part.at[m, PREV, hi], rfull.at[m, 1, hi], c_send.at[m, 1], c_recv.at[m, 1], to_xp)]

    def near_sum(m):
        return [remote(part.at[m, NEXT, hi], rfull.at[m, 0, hi], c_send.at[m, 2], c_recv.at[m, 2], to_xn),
                remote(part.at[m, PREV, lo], rfull.at[m, 1, lo], c_send.at[m, 3], c_recv.at[m, 3], to_xp)]

    tables = [pltpu.make_async_copy(src, dst, loc_sem.at[i]) for i, (src, dst) in enumerate((
        (ea, stage_e.at[0]), (sa, stage_s.at[0]), (ga, stage_g.at[0]),
        (eb, stage_e.at[1]), (sb, stage_s.at[1]), (gb, stage_g.at[1])))]
    local = [pltpu.make_async_copy(ta, tok.at[0, OWN], loc_sem.at[6]),
             pltpu.make_async_copy(tb, tok.at[1, OWN], loc_sem.at[7])]
    barrier = pltpu.get_barrier_semaphore()
    is_first, is_last = ty == 0, ty == tp_size - 1

    def greet(sem, dev):
        pl.semaphore_signal(sem, inc=1, device_id=dev, device_id_type=MESH)

    for dev in (to_xn, to_xp, to_pr):
        greet(barrier, dev)
    for cp in tables + local:
        cp.start()

    @pl.when(is_first)
    def _():
        pl.semaphore_wait(barrier, 3)
        greet(barrier, to_yn)
        greet(barrier, to_yp)

    @pl.when(jnp.logical_not(jnp.logical_or(is_first, is_last)))
    def _():
        pl.semaphore_wait(barrier, 4)
        greet(barrier, to_yn)
        greet(y_ready, to_yp)

    @pl.when(is_last)
    def _():
        pl.semaphore_wait(barrier, 5)
        greet(y_ready, to_yn)
        greet(y_ready, to_yp)
    first = own_sends(0)
    for cp in first[:2] + [to_partner(0, OWN)]:
        cp.start()
    for cp in tables:
        cp.wait()
    for m in range(2):
        kept = stage_s[m] >= 0
        ids = jnp.where(kept, stage_e[m] * cap + stage_s[m], -1).astype(jnp.float32)
        routing[OWN, pl.ds(2 * m * top_k, top_k)] = ids
        routing[OWN, pl.ds((2 * m + 1) * top_k, top_k)] = jnp.where(kept, stage_g[m], 0.0)
    for cp in weights(0, 0) + [meta_next, meta_prev, meta_pair[OWN]] + first[2:]:
        cp.start()
    for cp in local:
        cp.wait()

    row_id = lax.broadcasted_iota(jnp.int32, (exp_rows, rows), 0).astype(jnp.float32)

    def placed(ids, base, values):
        shifted = row_id + (base * exp_rows).astype(jnp.float32)
        total = jnp.zeros((exp_rows, rows), jnp.float32)
        for j in range(top_k):
            total = jnp.where(shifted == ids[j:j + 1, :], 1.0 if values is None else values[j:j + 1, :], total)
        return total

    def row_ids(k, m):
        return routing[k, pl.ds(2 * m * top_k, top_k), :]

    def gates(k, m):
        return routing[k, pl.ds((2 * m + 1) * top_k, top_k), :]

    def pass_tokens():
        first[0].wait_recv()
        first[1].wait_recv()
        for cp in (meta_next, meta_prev):
            cp.wait_recv()
        for cp in forwards(0) + meta_far + own_sends(1) + [meta_pair[NEXT], meta_pair[PREV], to_partner(1, OWN)]:
            cp.start()

        @pl.when(is_first)
        def _():
            pl.semaphore_wait(y_ready, 2)

        @pl.when(jnp.logical_not(jnp.logical_or(is_first, is_last)))
        def _():
            pl.semaphore_wait(y_ready, 1)
        for cp in y_own:
            cp.start()

    def arrivals(step):
        if step == 1:
            for cp in (meta_pair[OWN], to_partner(0, OWN)):
                cp.wait_recv()
        elif step == 2:
            first[2].wait_recv()
            first[3].wait_recv()
            to_partner(0, NEXT).start()
            to_partner(0, PREV).start()
        elif step in (3, 5):
            k = NEXT if step == 3 else PREV
            for cp in (meta_pair[k], to_partner(0, k)):
                cp.wait_recv()
        elif step == 6:
            for cp in meta_far:
                cp.wait_recv()
            meta_pair[FAR].start()
            for cp in forwards(0):
                cp.wait_recv()
            to_partner(0, FAR).start()
        elif step == 7:
            for cp in (meta_pair[FAR], to_partner(0, FAR)):
                cp.wait_recv()

    def pair_slot(block):
        return (block + 2) % 3 + block // 3

    def gather(m, first_step, last_step):
        def one(step, carry):
            if m == 0:
                for at in range(max(first_step, 1), last_step):
                    if at == 6:
                        continue
                    pl.when(step == at)(functools.partial(arrivals, at))
            block, other = step // 2, step % 2
            k = other * 4 + block
            place = placed(row_ids(k, m), ep, None).astype(jnp.bfloat16)
            got = jnp.dot(place, tok[m, k], preferred_element_type=jnp.float32).astype(jnp.bfloat16)
            at = (1 - other) * ((block + 1) % 4) + other * (4 + pair_slot(block))
            xr[:, at] = got.reshape(n_loc, cap, width)
            return carry
        lax.fori_loop(first_step, last_step, one, 0)

    def swiglu(x_rows, slot):
        proj_in = jnp.dot(x_rows, w1b[slot], preferred_element_type=jnp.float32)
        proj_gate = jnp.dot(x_rows, w3b[slot], preferred_element_type=jnp.float32)
        hidden = (jax.nn.silu(proj_in) * proj_gate).astype(jnp.bfloat16)
        return jnp.dot(hidden, w2b[slot], preferred_element_type=jnp.float32)

    def second_arrivals(step):
        sends = own_sends(1)
        if step == 0:
            sends[0].wait_recv()
            sends[1].wait_recv()
            for cp in forwards(1):
                cp.start()
        else:
            sends[2].wait_recv()
            sends[3].wait_recv()
            to_partner(1, NEXT).start()
            to_partner(1, PREV).start()

    early = n_loc // 2

    def run(e, slot, blocks):
        total = sum(b.size for b in blocks)
        x_rows = jnp.concatenate([xr[e, b].reshape(b.size * cap, width) for b in blocks], axis=0)
        res = swiglu(x_rows, slot).astype(jnp.bfloat16).reshape(total, cap, width)
        at = 0
        for b in blocks:
            xr[e, b] = res[at:at + b.size]
            at += b.size

    def stream(first, last, following, blocks, push, events=()):
        def one(e, carry):
            slot = e % 2
            for cp in weights(following(e), 1 - slot):
                cp.start()
            if push:
                @pl.when(e > 0)
                def _():
                    push_rows(0, e - 1).start()
            for cp in weights(e, slot):
                cp.wait()
            run(e, slot, blocks)
            for at, event in events:
                pl.when(e == at)(event)
            return carry
        lax.fori_loop(first, last, one, 0)

    def experts_first():
        own, far = [pl.ds(1, 1), pl.ds(6, 1)], [pl.ds(0, 1), pl.ds(7, 1)]
        near = [pl.ds(2, 4)]
        gather(0, 0, 2)
        stream(0, n_loc, lambda e: (e + 1) % n_loc, own, False, [(n_loc - 3, pass_tokens)])
        gather(0, 2, 6)
        stream(0, early, lambda e: (e + 1) % early, near, False, [(early - 2, functools.partial(arrivals, 6))])
        gather(0, 6, 8)
        stream(0, early, lambda e: e + 1, far, True, [(early - 1, functools.partial(second_arrivals, 0))])
        stream(early, n_loc, lambda e: (e + 1) % n_loc, [far[0]] + near + [far[1]], True)
        push_rows(0, n_loc - 1).start()

    def experts_second():
        def one(e, carry):
            slot = e % 2

            @pl.when(e < n_loc - 1)
            def _():
                for cp in weights(e + 1, 1 - slot):
                    cp.start()

            @pl.when(e > 0)
            def _():
                push_rows(1, e - 1).start()
            for cp in weights(e, slot):
                cp.wait()
            run(e, slot, [pl.ds(0, 8)])

            @pl.when(e == early)
            def _():
                for cp in y_own:
                    cp.wait_recv()
                for cp in y_far:
                    cp.start()
            return carry
        lax.fori_loop(0, n_loc, one, 0)
        push_rows(1, n_loc - 1).start()

    def combine(m):
        chunks = [pl.ds(n * 256, 256) for n in range(width // 256)]

        def weigh(gate_rows, rows_of, cols):
            acc = jnp.dot(gate_rows, rows_of(cols).reshape(exp_rows, 256), preferred_element_type=jnp.float32)
            return acc[0:rows] + acc[rows:2 * rows] + acc[2 * rows:3 * rows]

        def one(step, carry):
            i = 3 - step
            ids = row_ids(i, m)
            vals = gates(i, m)
            mine = jnp.concatenate(split_three(placed(ids, ep, vals).T), axis=0)
            other = jnp.concatenate(split_three(placed(ids, partner, vals).T), axis=0)
            at = (i + 1) % 4
            for cols in chunks:
                part[m, i, :, cols] = weigh(mine, lambda c: xr[:, at, :, c], cols)

            @pl.when(step == 0)
            def _():
                for e in range(n_loc):
                    push_rows(m, e).wait_recv()
            for cols in chunks:
                part[m, i, :, cols] += weigh(other, lambda c: rp[:, pair_slot(i), :, c], cols)

            @pl.when(step == 0)
            def _():
                for cp in first_far(m):
                    cp.start()

            @pl.when(step == 1)
            def _():
                near_own(m)[1].start()
                if m == 0:
                    second_arrivals(1)

            @pl.when(step == 2)
            def _():
                near_own(m)[0].start()
            return carry
        lax.fori_loop(0, 4, one, 0)

    def pass_on(m):
        incoming = first_far(m)
        sends = near_sum(m)
        incoming[0].wait_recv()
        part[m, NEXT, hi] = part[m, NEXT, hi] + rs1[m, 0]
        sends[0].start()
        incoming[1].wait_recv()
        part[m, PREV, lo] = part[m, PREV, lo] + rs1[m, 1]
        sends[1].start()

    def near_ready(m):
        for cp in near_own(m):
            cp.wait_recv()
        part[m, OWN, lo] += tok[m, OWN, lo].astype(jnp.float32) + rfull[m, 0, lo]
        part[m, OWN, hi] += tok[m, OWN, hi].astype(jnp.float32) + rfull[m, 1, hi]

    def finish(m, out):
        sums = near_sum(m)
        sums[0].wait_recv()
        out[hi] = (part[m, OWN, hi] + rfull[m, 0, hi]).astype(jnp.bfloat16)
        sums[1].wait_recv()
        out[lo] = (part[m, OWN, lo] + rfull[m, 1, lo]).astype(jnp.bfloat16)

    experts_first()
    combine(0)
    for cp in forwards(1):
        cp.wait_recv()
    to_partner(1, FAR).start()
    pl.semaphore_signal(free_sem, inc=1, device_id=to_pr, device_id_type=MESH)
    for k in range(4):
        to_partner(1, k).wait_recv()
    for e in range(n_loc):
        push_rows(0, e).wait_send()
    gather(1, 0, 8)
    pl.semaphore_wait(free_sem, 1)
    experts_second()
    pass_on(0)
    combine(1)
    for cp in y_far:
        cp.wait_recv()
    shared = []
    for slot, pair in enumerate((((s1, s3, s2), NEXT), (None, FAR))):
        srcs = [pair[0] or (g1.at[PREV - 1], g3.at[PREV - 1], g2.at[PREV - 1]), (g1.at[pair[1] - 1], g3.at[pair[1] - 1], g2.at[pair[1] - 1])]
        for p, (a1, a3, a2) in enumerate(srcs):
            part_of = pl.ds(p * sh, sh)
            shared.append(pltpu.make_async_copy(a1, w1b.at[slot, :, part_of], w_sem.at[slot, 3 + p]))
            shared.append(pltpu.make_async_copy(a3, w3b.at[slot, :, part_of], w_sem.at[slot, 5 + p]))
            shared.append(pltpu.make_async_copy(a2, w2b.at[slot, part_of, :], w_sem.at[slot, 7 + p]))
    for cp in shared:
        cp.start()
    for cp in shared:
        cp.wait()

    def shared_one(i, carry):
        m = i // 2
        part[m, OWN] = part[m, OWN] + swiglu(tok[m, OWN], i % 2)
        return carry
    lax.fori_loop(0, 4, shared_one, 0)

    near_ready(0)
    finish(0, out_a)
    pass_on(1)
    near_ready(1)
    finish(1, out_b)
    for m in range(2):
        for k in range(4):
            to_partner(m, k).wait_send()
        for cp in own_sends(m) + forwards(m) + first_far(m) + near_own(m) + near_sum(m):
            cp.wait_send()
    for e in range(n_loc):
        push_rows(1, e).wait_send()
    for cp in [meta_next, meta_prev] + meta_far + meta_pair + y_own + y_far:
        cp.wait_send()


def place_kernel(a, b, out_a, out_b, sem):
    copies = [pltpu.make_async_copy(a, out_a, sem.at[0]), pltpu.make_async_copy(b, out_b, sem.at[1])]
    for cp in copies:
        cp.start()
    for cp in copies:
        cp.wait()


def solution(mesh):
    ep_size = mesh.shape['ep']
    tp_size = mesh.shape['tp']
    tok_spec = P(('data', 'ep', 'tp'), None)
    in_specs = (tok_spec,) * 8 + (P(None, 'tp'), P(None, 'tp'), P('tp', None), P('ep', None, None), P('ep', None, None), P('ep', None, None))

    def layer_local(tokens_a, tokens_b, experts_a, experts_b, gates_a, gates_b, slots_a, slots_b, shared_w1, shared_w3, shared_w2, routed_w1, routed_w3, routed_w2):
        rows, width = tokens_a.shape
        top_k = experts_a.shape[1]
        n_loc, _, ff = routed_w1.shape
        sh = shared_w1.shape[1]
        cap = capacity_rows(rows, top_k, n_loc * ep_size)
        half = rows // 2
        tables = [a.T for a in (experts_a, experts_b, gates_a, gates_b, slots_a, slots_b)]
        bf, f32 = jnp.bfloat16, jnp.float32
        dma = pltpu.SemaphoreType.DMA
        any_spec = pl.BlockSpec(memory_space=pl.ANY)
        vmem_spec = pl.BlockSpec(memory_space=pltpu.VMEM)
        outs = pl.pallas_call(
            functools.partial(layer_kernel, (top_k, ep_size, tp_size, cap)),
            out_shape=(pltpu.VMEM((rows, width), bf), pltpu.VMEM((rows, width), bf),
                       jax.ShapeDtypeStruct((3, width, sh), bf), jax.ShapeDtypeStruct((3, width, sh), bf),
                       jax.ShapeDtypeStruct((3, sh, width), bf)),
            in_specs=[any_spec] * 14,
            out_specs=[vmem_spec] * 2 + [any_spec] * 3,
            scratch_shapes=[
                pltpu.VMEM((2, 8, rows, width), bf),
                pltpu.VMEM((8, 4 * top_k, rows), f32),
                pltpu.VMEM((2, top_k, rows), jnp.int32),
                pltpu.VMEM((2, top_k, rows), jnp.int32),
                pltpu.VMEM((2, top_k, rows), f32),
                pltpu.VMEM((n_loc, 8, cap, width), bf),
                pltpu.VMEM((n_loc, 4, cap, width), bf),
                pltpu.VMEM((2, width, ff), bf),
                pltpu.VMEM((2, width, ff), bf),
                pltpu.VMEM((2, ff, width), bf),
                pltpu.VMEM((2, 4, rows, width), f32),
                pltpu.VMEM((2, 2, half, width), f32),
                pltpu.VMEM((2, 2, rows, width), f32),
                dma((8,)), dma((2, 9)), dma((2, 6)), dma((2, 6)), dma((2, 4)), dma((2, 4)), dma((8,)), dma((8,)),
                dma((9,)), dma((9,)), dma((2, n_loc)), dma((2, n_loc)), dma((2, 6)), dma((2, 6)),
                pltpu.SemaphoreType.REGULAR, pltpu.SemaphoreType.REGULAR,
            ],
            compiler_params=pltpu.CompilerParams(collective_id=0, has_side_effects=True, vmem_limit_bytes=VMEM_BYTES),
        )(*tables, tokens_a, tokens_b, shared_w1, shared_w3, shared_w2, routed_w1, routed_w3, routed_w2)
        held = outs[:2]
        return pl.pallas_call(
            place_kernel,
            out_shape=(jax.ShapeDtypeStruct((rows, width), bf),) * 2,
            in_specs=[vmem_spec] * 2,
            out_specs=[any_spec] * 2,
            scratch_shapes=[dma((2,))],
            compiler_params=pltpu.CompilerParams(vmem_limit_bytes=1 << 20),
        )(*held)

    return jax.shard_map(layer_local, mesh=mesh, in_specs=in_specs, out_specs=(tok_spec, tok_spec), check_vma=False)
```
